128 devices in a mesh: grp: 4 (over x), tile: 32 (over y, z, core).
Axes of the slice: x: 4, y: 4, z: 4, core: 2. Of those that a mesh axis runs over, the one named last changes fastest.
Arguments:
- descriptors: bfloat16 [64, 4096, 256], P('grp', 'tile'), may hold values from -8 to 8
- pairs: int32 [32, 2], P('grp'), may hold values from 0 to 63, as said below
- counts: int32 [64], replicated, may hold values from 1024 to 4096
Outputs:
- row_lse: float32 [32, 4096], P('grp', 'tile')
- col_lse: float32 [32, 4096], P('grp', 'tile')
- best_log: float32 [32, 4096], P('grp', 'tile')
The draws below stay inside these ranges and needn't reach their ends.
Inputs may be any that keep to these rules, and one draw needn't show every extreme that they name: `pairs`: the two images of a pair differ.
All inputs are finite; a program needn't handle non-finite values.
Results may differ from the reference program's by a relative error of at most 0.0003.
Values may be sent and summed in bfloat16 or wider, within the bound.
A program may use at most 64 MiB of HBM per device.

```python
import math
import jax
import jax.numpy as jnp
from jax import lax

D = 256
KP = 4096
NIMG = 64
PAIRS = 32


def draw_descriptors(key, part):
    base = jax.random.normal(key, (NIMG, KP, D), jnp.float32)
    return jnp.clip(base, -8.0, 8.0).astype(jnp.bfloat16)


def draw_pairs(key, part):
    first_key = jax.random.fold_in(key, 21)
    step_key = jax.random.fold_in(key, 22)
    first_image = jax.random.randint(first_key, (PAIRS,), 0, NIMG)
    stride = jax.random.randint(step_key, (PAIRS,), 1, NIMG)
    second = (first_image + stride) % NIMG
    return jnp.stack([first_image, second], axis=1).astype(jnp.int32)


def plant(drawn, key, least, top_value):
    spot = [jax.random.randint(jax.random.fold_in(key, axis), (), 0, length) for axis, length in enumerate(drawn.shape)]
    longest = drawn.shape.index(max(drawn.shape))
    beside = spot[:longest] + [(spot[longest] + 1) % drawn.shape[longest]] + spot[longest + 1:]
    return drawn.at[tuple(spot)].set(least).at[tuple(beside)].set(top_value)


def setup_inputs(seed: int = 0) -> dict:
    arg_keys = jax.random.split(jax.random.key(seed), 4)
    return {
        "descriptors": draw_descriptors(jax.random.fold_in(arg_keys[3], 71), 0),
        "pairs": draw_pairs(jax.random.fold_in(arg_keys[3], 71), 0),
        "counts": plant(jax.random.randint(arg_keys[2], (NIMG,), KP // 4, KP + 1), jax.random.fold_in(arg_keys[2], 1), KP // 4, KP).astype(jnp.int32),
    }


NEGATIVE = -1e+30

def masked_logsumexp(scores, valid, axis):
    highest = lax.optimization_barrier(jnp.max(jnp.where(valid, scores, NEGATIVE), axis=axis, keepdims=True))
    summed = lax.optimization_barrier(jnp.sum(jnp.where(valid, jnp.exp(scores - highest), 0.0), axis=axis))
    return jnp.squeeze(highest, axis) + jnp.log(summed)

def reference(descriptors, pairs, counts):
    score_scale = 2.0 / math.sqrt(D)
    positions = jnp.arange(KP, dtype=jnp.int32)

    def one_pair(pair_row):
        query_image = descriptors[pair_row[0]]
        key_image = descriptors[pair_row[1]]
        query_valid = positions < counts[pair_row[0]]
        key_valid = positions < counts[pair_row[1]]
        scores = jnp.dot(query_image, key_image.T, preferred_element_type=jnp.float32) * score_scale
        row_values = masked_logsumexp(scores, key_valid[None, :], 1)
        col_values = masked_logsumexp(scores, query_valid[:, None], 0)
        best_values = lax.optimization_barrier(jnp.max(jnp.where(key_valid[None, :], 2.0 * scores - col_values[None, :], NEGATIVE), axis=1)) - row_values
        return (jnp.where(query_valid, row_values, 0.0), jnp.where(key_valid, col_values, 0.0), jnp.where(query_valid, best_values, 0.0))
    results = lax.map(one_pair, pairs)
    return (results[0], results[1], results[2])
```

```python
import functools
import math

import jax
import jax.numpy as jnp
from jax import lax
from jax.experimental import pallas as pl
from jax.experimental.pallas import tpu as pltpu
from jax.sharding import Mesh
from jax.sharding import PartitionSpec as P

TILE = ("tile_0", "tile_1", "tile_2")
MESH = pl.DeviceIdType.MESH

NEGATIVE = -1e30
CHUNKS = 8
ROWS = 16
GROUPS = 4
IMAGES = 16
SOURCES = 8
MEMBERS = 4
LOG2E = math.log2(math.e)
LN2 = math.log(2.0)


def slot_index(z, core, chunk, lane):
    outer = jnp.logical_or(z == 0, z == 3)
    low = jnp.where(outer, 0, 1)
    high = jnp.where(outer, 3, 2)
    source = lane // ROWS
    z_source = jnp.where(source % 2 == 0, low, high)
    tile = (source // 2) * 8 + z_source * 2 + core
    return tile * (CHUNKS * ROWS) + chunk * ROWS + lane % ROWS


def block_transpose(x):
    sub = lax.broadcasted_iota(jnp.int32, (8, 128), 0)
    block = lax.broadcasted_iota(jnp.int32, (8, 128), 1) // ROWS
    out = x
    for d in range(8):
        moved = x if d == 0 else pltpu.roll(pltpu.roll(x, ROWS * d, 1), 8 - d, 0)
        out = jnp.where(block == (sub + d) % 8, moved, out)
    return out


def kernel(scale, pairs, counts, desc, out_row, out_col, out_best, *scratch):
    gathered = scratch[:CHUNKS]
    staged = scratch[CHUNKS : 2 * CHUNKS]
    (
        queries, keys, scores, row_top, row_sum, col_top, col_sum, key_bias, query_bias,
        stats, stats_got, col_full, best_cols, sent, got,
        load_sem, xs, xr, qs, qr, ks, kr, fs, fr, cs, cr, vs, vr, os_, or_,
    ) = scratch[2 * CHUNKS :]
    x, y, z, c = (lax.axis_index(a) for a in ("grp",) + TILE)
    right = (lax.rem(x + 1, 4), y, z, c)
    left = (lax.rem(x + 3, 4), y, z, c)
    half = z // 2
    parity = z % 2
    place = y * 2 + half
    member = parity * 2 + c
    z_beside = half * 2 + (1 - parity)
    beside = (x, y, z_beside, c)
    sibling = (x, y, z, 1 - c)
    diagonal = (x, y, z_beside, 1 - c)
    member_beside = (1 - parity) * 2 + c

    def peer(dy, dk):
        return (x, lax.rem(y + dy, 4), z if dk == 0 else 3 - z, c)

    def peer_place(dy, dk):
        return lax.rem(y + dy, 4) * 2 + (half if dk == 0 else 1 - half)

    loads = [
        pltpu.make_async_copy(
            desc.at[:, pl.ds(r * ROWS, ROWS), :], gathered[r].at[pl.ds(0, IMAGES)], load_sem.at[r]
        )
        for r in range(CHUNKS)
    ]
    for load in loads:
        load.start()

    others = [(dy, dk) for dy in range(4) for dk in range(2) if (dy, dk) != (0, 0)]
    barrier = pltpu.get_barrier_semaphore()
    greeted = [right, left, beside, sibling, diagonal] + [peer(dy, dk) for dy, dk in others]
    for device in greeted:
        pl.semaphore_signal(barrier, inc=1, device_id=device, device_id_type=MESH)

    p = place
    query_count = counts[pairs[p, 0]]
    key_count = counts[pairs[p, 1]]
    row_top[...] = jnp.full(row_top.shape, NEGATIVE, jnp.float32)
    row_sum[...] = jnp.zeros(row_sum.shape, jnp.float32)
    col_top[...] = jnp.full(col_top.shape, NEGATIVE, jnp.float32)
    col_sum[...] = jnp.zeros(col_sum.shape, jnp.float32)
    for r in range(CHUNKS):
        lane = lax.broadcasted_iota(jnp.int32, (1, 128), 1)
        for m in range(MEMBERS):
            index = slot_index(half * 2 + m // 2, m % 2, r, lane)
            key_bias[r, :, pl.ds(m * 128, 128)] = jnp.where(index < key_count, 0.0, NEGATIVE)
        sub = lax.broadcasted_iota(jnp.int32, (128, 128), 0)
        query_bias[r] = jnp.where(slot_index(z, c, r, sub) < query_count, 0.0, NEGATIVE)

    pl.semaphore_wait(barrier, len(greeted))

    def remote(src, dst, send, recv, device):
        return pltpu.make_async_remote_copy(
            src_ref=src, dst_ref=dst, send_sem=send, recv_sem=recv,
            device_id=device, device_id_type=MESH,
        )

    started = []

    def go(copy):
        copy.start()
        started.append(copy)

    def own(r):
        return gathered[r].at[pl.ds(0, IMAGES)]

    from_left = lambda r: gathered[r].at[pl.ds(16, 16)]
    from_right = lambda r: gathered[r].at[pl.ds(48, 16)]
    far_low = lambda r: gathered[r].at[pl.ds(32, 8)]
    far_high = lambda r: gathered[r].at[pl.ds(40, 8)]

    def x_first(r):
        loads[r].wait()
        go(remote(own(r), from_left(r), xs.at[0, r], xr.at[0, r], right))
        go(remote(own(r), from_right(r), xs.at[1, r], xr.at[1, r], left))

    def landed(ref, send, recv):
        remote(ref, ref, send, recv, right).wait_recv()

    def x_second(r):
        landed(from_left(r), xs.at[0, r], xr.at[0, r])
        go(remote(gathered[r].at[pl.ds(16, 8)], far_low(r), xs.at[2, r], xr.at[2, r], right))
        landed(from_right(r), xs.at[1, r], xr.at[1, r])
        go(remote(gathered[r].at[pl.ds(56, 8)], far_high(r), xs.at[3, r], xr.at[3, r], left))

    def select(r):
        landed(far_low(r), xs.at[2, r], xr.at[2, r])
        landed(far_high(r), xs.at[3, r], xr.at[3, r])
        for pair in range(8):
            for side in range(2):
                image = pairs[pair, side]
                turn = lax.rem(x + 4 - image // IMAGES, 4)
                staged[r][pair, side] = gathered[r][turn * IMAGES + image % IMAGES]

    def spread(r):
        for dy in range(4):
            for dk in range(2):
                to = peer_place(dy, dk)
                e = dy * 2 + dk
                z_to = z if dk == 0 else 3 - z
                m_to = (z_to % 2) * 2 + c
                q_src, k_src = staged[r].at[to, 0], staged[r].at[to, 1]
                q_dst, k_dst = queries.at[r, place], keys.at[r, m_to, place]
                if e == 0:
                    for copy in (
                        pltpu.make_async_copy(q_src, q_dst, qr.at[r, place]),
                        pltpu.make_async_copy(k_src, k_dst, kr.at[r, place]),
                    ):
                        copy.start()
                else:
                    go(remote(k_src, k_dst, ks.at[r, e], kr.at[r, place], peer(dy, dk)))
                    go(remote(q_src, q_dst, qs.at[r, e], qr.at[r, place], peer(dy, dk)))

    def pass_keys(r):
        for s in range(SOURCES):
            landed(keys.at[r, member, s], ks.at[r, 0], kr.at[r, s])
        block = keys.at[r, member]
        go(remote(block, block, fs.at[0, r], fr.at[0, r], beside))
        go(remote(block, block, fs.at[1, r], fr.at[1, r], sibling))

    def pass_again(r):
        block = keys.at[r, member_beside]
        landed(block, fs.at[0, r], fr.at[0, r])
        go(remote(block, block, fs.at[2, r], fr.at[2, r], sibling))

    def tile(qi, kj):
        q = queries[qi].reshape(128, 256)
        k = keys[kj].reshape(512, 256)
        s = lax.dot_general(q, k, (((1,), (1,)), ((), ())), preferred_element_type=jnp.float32)
        kb = key_bias[kj]
        top = col_top[kj]
        tops = []
        high = top
        for g in range(8):
            rows = pl.ds(g * 16, 16)
            t = s[g * 16 : (g + 1) * 16] * scale + kb
            qb = query_bias[qi, rows, :]
            parts = [t[:, i * 128 : (i + 1) * 128] + qb for i in range(4)]
            for i in range(4):
                scores[qi, kj, rows, pl.ds(i * 128, 128)] = parts[i]
            tops.append(
                jnp.maximum(jnp.maximum(parts[0], parts[1]), jnp.maximum(parts[2], parts[3]))
            )
            both = jnp.concatenate(parts, axis=1)
            high = jnp.maximum(high, jnp.maximum(both[:8], both[8:]))
        total = col_sum[kj] * jnp.exp2(top - high)
        for g in range(8):
            rows = pl.ds(g * 16, 16)
            t = scores[qi, kj, rows, :]
            before = row_top[qi, rows, :]
            now = jnp.maximum(before, tops[g])
            acc = row_sum[qi, rows, :] * jnp.exp2(before - now)
            for i in range(4):
                acc += jnp.exp2(t[:, i * 128 : (i + 1) * 128] - now)
            row_sum[qi, rows, :] = acc
            row_top[qi, rows, :] = now
            total += jnp.exp2(t[:8] - high) + jnp.exp2(t[8:] - high)
        col_sum[kj] = total
        col_top[kj] = high

    def first_pass(r):
        for s in range(SOURCES):
            landed(queries.at[r, s], qs.at[r, 0], qr.at[r, s])
        landed(keys.at[r, parity * 2 + 1 - c], fs.at[1, r], fr.at[1, r])
        landed(keys.at[r, (1 - parity) * 2 + 1 - c], fs.at[2, r], fr.at[2, r])

        def body(n, carry):
            tile(jnp.minimum(n, r), jnp.where(n <= r, r, n - r - 1))
            return carry

        lax.fori_loop(0, 2 * r + 1, body, 0)

    x_first(0)
    x_first(1)
    for i in range(CHUNKS + 4):
        if i < CHUNKS:
            x_second(i)
            if i + 2 < CHUNKS:
                x_first(i + 2)
        if 0 <= i - 1 < CHUNKS:
            select(i - 1)
            spread(i - 1)
        if 0 <= i - 2 < CHUNKS:
            pass_keys(i - 2)
        if 0 <= i - 3 < CHUNKS:
            pass_again(i - 3)
        if 0 <= i - 4 < CHUNKS:
            first_pass(i - 4)

    for kj in range(CHUNKS):
        top = jnp.max(col_top[kj], axis=0, keepdims=True)
        total = jnp.sum(col_sum[kj] * jnp.exp2(col_top[kj] - top), axis=0, keepdims=True)
        for m in range(MEMBERS):
            stats[m, 0, pl.ds(kj, 1), :] = top[:, m * 128 : (m + 1) * 128]
            stats[m, 1, pl.ds(kj, 1), :] = total[:, m * 128 : (m + 1) * 128]
    team = [(1, sibling), (2, beside), (3, diagonal)]

    def mate(e):
        dh, dc = e // 2, e % 2
        return (1 - parity if dh else parity) * 2 + (1 - c if dc else c)

    for e, device in team:
        go(remote(stats.at[mate(e)], stats_got.at[member], cs.at[e], cr.at[e], device))

    lane = lax.broadcasted_iota(jnp.int32, (128, 128), 1)
    row_cols = jnp.zeros((128, 128), jnp.float32)
    for qi in range(CHUNKS):
        top = jnp.max(row_top[qi], axis=1, keepdims=True)
        total = jnp.sum(row_sum[qi] * jnp.exp2(row_top[qi] - top), axis=1, keepdims=True)
        row_cols = jnp.where(lane == qi, top + jnp.log2(total), row_cols)
    row_log = jnp.transpose(row_cols)[:8]

    for e, _ in team:
        landed(stats_got.at[mate(e)], cs.at[e], cr.at[e])
    tops = [stats[member, 0]] + [stats_got[mate(e), 0] for e, _ in team]
    sums = [stats[member, 1]] + [stats_got[mate(e), 1] for e, _ in team]
    highest = functools.reduce(jnp.maximum, tops)
    total = sum(b * jnp.exp2(a - highest) for a, b in zip(tops, sums))
    own_col = highest + jnp.log2(total)
    col_full[member] = own_col
    for e, device in team:
        go(remote(col_full.at[member], col_full.at[member], vs.at[e], vr.at[e], device))
    for e, _ in team:
        landed(col_full.at[mate(e)], vs.at[e], vr.at[e])

    def second(qi, carry):
        best = [None] * 8
        for kj in range(CHUNKS):
            halves = [col_full[m, pl.ds(kj, 1), :] * 0.5 for m in range(MEMBERS)]
            for g in range(8):
                t = scores[qi, kj, pl.ds(g * 16, 16), :]
                parts = [t[:, m * 128 : (m + 1) * 128] - halves[m] for m in range(MEMBERS)]
                part = jnp.maximum(
                    jnp.maximum(parts[0], parts[1]), jnp.maximum(parts[2], parts[3])
                )
                best[g] = part if kj == 0 else jnp.maximum(best[g], part)
        for g in range(8):
            rows = pl.ds(g * 16, 16)
            most = jnp.max(best[g], axis=1, keepdims=True)
            best_cols[rows, :] = jnp.where(lane[:16] == qi, most, best_cols[rows, :])
        return carry

    best_cols[...] = jnp.zeros((128, 128), jnp.float32)
    lax.fori_loop(0, CHUNKS, second, 0)
    best = 2.0 * jnp.transpose(best_cols[...])[:8] - row_log

    chunk = lax.broadcasted_iota(jnp.int32, (8, 128), 0)
    lane8 = lax.broadcasted_iota(jnp.int32, (8, 128), 1)
    index = slot_index(z, c, chunk, lane8)
    query_valid = index < query_count
    results = (
        jnp.where(query_valid, row_log * LN2, 0.0),
        jnp.where(index < key_count, own_col * LN2, 0.0),
        jnp.where(query_valid, best * LN2, 0.0),
    )
    for j, value in enumerate(results):
        value = block_transpose(value)
        for s in range(SOURCES):
            sent[s, pl.ds(j, 1), :] = value[s : s + 1]
    for dy in range(4):
        for dk in range(2):
            e = dy * 2 + dk
            to = peer_place(dy, dk)
            if e == 0:
                pltpu.make_async_copy(sent.at[to], got.at[place], or_.at[place]).start()
            else:
                go(remote(sent.at[to], got.at[place], os_.at[e], or_.at[place], peer(dy, dk)))
    for s in range(SOURCES):
        landed(got.at[s], os_.at[0], or_.at[s])
    for s in range(SOURCES):
        out_row[pl.ds(s, 1), :] = got[s, pl.ds(0, 1), :]
        out_col[pl.ds(s, 1), :] = got[s, pl.ds(1, 1), :]
        out_best[pl.ds(s, 1), :] = got[s, pl.ds(2, 1), :]
    for copy in started:
        copy.wait_send()


def local(descriptors, pairs, counts):
    scale = 2.0 / math.sqrt(descriptors.shape[2]) * LOG2E
    width = descriptors.shape[2]
    bf16, f32 = jnp.bfloat16, jnp.float32
    dma = pltpu.SemaphoreType.DMA
    scratch = [pltpu.VMEM((GROUPS * IMAGES, ROWS, width), bf16) for _ in range(CHUNKS)]
    scratch += [pltpu.VMEM((8, 2, ROWS, width), bf16) for _ in range(CHUNKS)]
    scratch += [
        pltpu.VMEM((CHUNKS, SOURCES, ROWS, width), bf16),
        pltpu.VMEM((CHUNKS, MEMBERS, SOURCES, ROWS, width), bf16),
        pltpu.VMEM((CHUNKS, CHUNKS, 128, 512), f32),
        pltpu.VMEM((CHUNKS, 128, 128), f32),
        pltpu.VMEM((CHUNKS, 128, 128), f32),
        pltpu.VMEM((CHUNKS, 8, 512), f32),
        pltpu.VMEM((CHUNKS, 8, 512), f32),
        pltpu.VMEM((CHUNKS, 1, 512), f32),
        pltpu.VMEM((CHUNKS, 128, 128), f32),
        pltpu.VMEM((MEMBERS, 2, 8, 128), f32),
        pltpu.VMEM((MEMBERS, 2, 8, 128), f32),
        pltpu.VMEM((MEMBERS, 8, 128), f32),
        pltpu.VMEM((128, 128), f32),
        pltpu.VMEM((8, 8, 128), f32),
        pltpu.VMEM((8, 8, 128), f32),
        dma((CHUNKS,)),
        dma((4, CHUNKS)), dma((4, CHUNKS)),
        dma((CHUNKS, 8)), dma((CHUNKS, 8)),
        dma((CHUNKS, 8)), dma((CHUNKS, 8)),
        dma((3, CHUNKS)), dma((3, CHUNKS)),
        dma((4,)), dma((4,)),
        dma((4,)), dma((4,)),
        dma((8,)), dma((8,)),
    ]
    out = jax.ShapeDtypeStruct((8, 128), f32)
    return pl.pallas_call(
        functools.partial(kernel, scale),
        out_shape=(out, out, out),
        in_specs=[
            pl.BlockSpec(memory_space=pltpu.SMEM),
            pl.BlockSpec(memory_space=pltpu.SMEM),
            pl.BlockSpec(memory_space=pl.ANY),
        ],
        out_specs=[pl.BlockSpec(memory_space=pltpu.VMEM)] * 3,
        scratch_shapes=scratch,
        compiler_params=pltpu.CompilerParams(
            collective_id=0, has_side_effects=True, vmem_limit_bytes=48 * 1024 * 1024
        ),
    )(pairs, counts, descriptors)


def solution(mesh):
    torus = Mesh(
        mesh.devices.reshape(mesh.shape["grp"], 4, 4, 2), ("grp", "tile_0", "tile_1", "tile_2")
    )
    return jax.shard_map(
        local,
        mesh=torus,
        in_specs=(P("grp", TILE, None), P("grp", None), P()),
        out_specs=(P("grp", TILE), P("grp", TILE), P("grp", TILE)),
        check_vma=False,
    )
```

```python
import functools
import math

import jax
import jax.numpy as jnp
from jax import lax
from jax.experimental import pallas as pl
from jax.experimental.pallas import tpu as pltpu
from jax.sharding import Mesh
from jax.sharding import PartitionSpec as P

TILE = ("tile_0", "tile_1", "tile_2")
MESH = pl.DeviceIdType.MESH

NEGATIVE = -1e30
CHUNKS = 8
ROWS = 16
GROUPS = 4
IMAGES = 16
SOURCES = 8
MEMBERS = 4
LOG2E = math.log2(math.e)
LN2 = math.log(2.0)


def slot_index(z, core, chunk, lane):
    outer = jnp.logical_or(z == 0, z == 3)
    low = jnp.where(outer, 0, 1)
    high = jnp.where(outer, 3, 2)
    source = lane // ROWS
    z_source = jnp.where(source % 2 == 0, low, high)
    tile = (source // 2) * 8 + z_source * 2 + core
    return tile * (CHUNKS * ROWS) + chunk * ROWS + lane % ROWS


def block_transpose(x):
    sub = lax.broadcasted_iota(jnp.int32, (8, 128), 0)
    block = lax.broadcasted_iota(jnp.int32, (8, 128), 1) // ROWS
    out = x
    for d in range(8):
        moved = x if d == 0 else pltpu.roll(pltpu.roll(x, ROWS * d, 1), 8 - d, 0)
        out = jnp.where(block == (sub + d) % 8, moved, out)
    return out


def kernel(scale, pairs, counts, desc, out, *scratch):
    gathered = scratch[:CHUNKS]
    staged = scratch[CHUNKS : 2 * CHUNKS]
    (
        queries, keys, scores, row_top, row_sum, col_top, col_sum, key_bias, query_bias,
        col_log, col_half, best_cols, held_even, held_odd, sent, got,
        load_sem, xs, xr, qs, qr, ks, kr, fs, fr, cs, cr, os_, or_,
    ) = scratch[2 * CHUNKS :]
    x, y, z, c = (lax.axis_index(a) for a in ("grp",) + TILE)
    right = (lax.rem(x + 1, 4), y, z, c)
    left = (lax.rem(x + 3, 4), y, z, c)
    half = z // 2
    parity = z % 2
    place = y * 2 + half
    member = parity * 2 + c
    z_beside = half * 2 + (1 - parity)
    beside = (x, y, z_beside, c)
    sibling = (x, y, z, 1 - c)
    diagonal = (x, y, z_beside, 1 - c)
    member_beside = (1 - parity) * 2 + c

    def peer(dy, dk):
        return (x, lax.rem(y + dy, 4), z if dk == 0 else 3 - z, c)

    def peer_place(dy, dk):
        return lax.rem(y + dy, 4) * 2 + (half if dk == 0 else 1 - half)

    loads = [
        pltpu.make_async_copy(
            desc.at[:, pl.ds(r * ROWS, ROWS), :], gathered[r].at[pl.ds(0, IMAGES)], load_sem.at[r]
        )
        for r in range(CHUNKS)
    ]
    for load in loads:
        load.start()

    others = [(dy, dk) for dy in range(4) for dk in range(2) if (dy, dk) != (0, 0)]
    barrier = pltpu.get_barrier_semaphore()
    greeted = [right, left, beside, sibling, diagonal] + [peer(dy, dk) for dy, dk in others]
    for device in greeted:
        pl.semaphore_signal(barrier, inc=1, device_id=device, device_id_type=MESH)

    p = place
    query_count = counts[pairs[0, p]]
    key_count = counts[pairs[1, p]]
    row_top[...] = jnp.full(row_top.shape, NEGATIVE, jnp.float32)
    row_sum[...] = jnp.zeros(row_sum.shape, jnp.float32)
    col_top[...] = jnp.full(col_top.shape, NEGATIVE, jnp.float32)
    col_sum[...] = jnp.zeros(col_sum.shape, jnp.float32)
    for r in range(CHUNKS):
        lane = lax.broadcasted_iota(jnp.int32, (1, 128), 1)
        for m in range(MEMBERS):
            index = slot_index(half * 2 + m // 2, m % 2, r, lane)
            key_bias[r, :, pl.ds(m * 128, 128)] = jnp.where(index < key_count, 0.0, NEGATIVE)
        sub = lax.broadcasted_iota(jnp.int32, (128, 128), 0)
        query_bias[r] = jnp.where(slot_index(z, c, r, sub) < query_count, 0.0, NEGATIVE)

    pl.semaphore_wait(barrier, len(greeted))

    def remote(src, dst, send, recv, device):
        return pltpu.make_async_remote_copy(
            src_ref=src, dst_ref=dst, send_sem=send, recv_sem=recv,
            device_id=device, device_id_type=MESH,
        )

    started = []

    def go(copy):
        copy.start()
        started.append(copy)

    def own(r):
        return gathered[r].at[pl.ds(0, IMAGES)]

    from_left = lambda r: gathered[r].at[pl.ds(16, 16)]
    from_right = lambda r: gathered[r].at[pl.ds(48, 16)]
    far_low = lambda r: gathered[r].at[pl.ds(32, 8)]
    far_high = lambda r: gathered[r].at[pl.ds(40, 8)]

    def x_first(r):
        loads[r].wait()
        go(remote(own(r), from_left(r), xs.at[0, r], xr.at[0, r], right))
        go(remote(own(r), from_right(r), xs.at[1, r], xr.at[1, r], left))

    def landed(ref, send, recv):
        remote(ref, ref, send, recv, right).wait_recv()

    def x_second(r):
        landed(from_left(r), xs.at[0, r], xr.at[0, r])
        go(remote(gathered[r].at[pl.ds(16, 8)], far_low(r), xs.at[2, r], xr.at[2, r], right))
        landed(from_right(r), xs.at[1, r], xr.at[1, r])
        go(remote(gathered[r].at[pl.ds(56, 8)], far_high(r), xs.at[3, r], xr.at[3, r], left))

    def select(r):
        landed(far_low(r), xs.at[2, r], xr.at[2, r])
        landed(far_high(r), xs.at[3, r], xr.at[3, r])
        for pair in range(8):
            for side in range(2):
                image = pairs[side, pair]
                turn = lax.rem(x + 4 - image // IMAGES, 4)
                staged[r][pair, side] = gathered[r][turn * IMAGES + image % IMAGES]

    def spread(r):
        for dy in range(4):
            for dk in range(2):
                to = peer_place(dy, dk)
                e = dy * 2 + dk
                z_to = z if dk == 0 else 3 - z
                m_to = (z_to % 2) * 2 + c
                q_src, k_src = staged[r].at[to, 0], staged[r].at[to, 1]
                q_dst, k_dst = queries.at[r, place], keys.at[r, m_to, place]
                if e == 0:
                    for copy in (
                        pltpu.make_async_copy(q_src, q_dst, qr.at[r, place]),
                        pltpu.make_async_copy(k_src, k_dst, kr.at[r, place]),
                    ):
                        copy.start()
                else:
                    go(remote(k_src, k_dst, ks.at[r, e], kr.at[r, place], peer(dy, dk)))
                    go(remote(q_src, q_dst, qs.at[r, e], qr.at[r, place], peer(dy, dk)))

    def pass_keys(r):
        for s in range(SOURCES):
            landed(keys.at[r, member, s], ks.at[r, 0], kr.at[r, s])
        block = keys.at[r, member]
        go(remote(block, block, fs.at[0, r], fr.at[0, r], beside))
        go(remote(block, block, fs.at[1, r], fr.at[1, r], sibling))

    def pass_again(r):
        block = keys.at[r, member_beside]
        landed(block, fs.at[0, r], fr.at[0, r])
        go(remote(block, block, fs.at[2, r], fr.at[2, r], sibling))

    def product(qi, kj, held):
        q = queries[qi].reshape(128, 256)
        k = keys[kj].reshape(512, 256)
        held[...] = lax.dot_general(
            q, k, (((1,), (1,)), ((), ())), preferred_element_type=jnp.float32
        )

    def fold(qi, kj, held):
        kb = key_bias[kj]
        top = col_top[kj]
        tops = []
        high = top
        for g in range(8):
            rows = pl.ds(g * 16, 16)
            t = held[rows, :] * scale + kb
            qb = query_bias[qi, rows, :]
            parts = [t[:, i * 128 : (i + 1) * 128] + qb for i in range(4)]
            tops.append(
                jnp.maximum(jnp.maximum(parts[0], parts[1]), jnp.maximum(parts[2], parts[3]))
            )
            both = jnp.concatenate(parts, axis=1)
            scores[qi, kj, rows, :] = both
            held[rows, :] = both
            high = jnp.maximum(high, jnp.maximum(both[:8], both[8:]))
        total = col_sum[kj] * jnp.exp2(top - high)
        for g in range(8):
            rows = pl.ds(g * 16, 16)
            t = held[rows, :]
            before = row_top[qi, rows, :]
            now = jnp.maximum(before, tops[g])
            acc = row_sum[qi, rows, :] * jnp.exp2(before - now)
            for i in range(4):
                acc += jnp.exp2(t[:, i * 128 : (i + 1) * 128] - now)
            row_sum[qi, rows, :] = acc
            row_top[qi, rows, :] = now
            total += jnp.exp2(t[:8] - high) + jnp.exp2(t[8:] - high)
        col_sum[kj] = total
        col_top[kj] = high

    def first_pass(r):
        for s in range(SOURCES):
            landed(queries.at[r, s], qs.at[r, 0], qr.at[r, s])
        landed(keys.at[r, parity * 2 + 1 - c], fs.at[1, r], fr.at[1, r])
        landed(keys.at[r, (1 - parity) * 2 + 1 - c], fs.at[2, r], fr.at[2, r])

        def at(n):
            return jnp.minimum(n, r), jnp.where(n <= r, r, n - r - 1)

        def body(n, carry):
            product(*at(2 * n + 1), held_odd)
            fold(*at(2 * n), held_even)
            product(*at(2 * n + 2), held_even)
            fold(*at(2 * n + 1), held_odd)
            return carry

        product(*at(0), held_even)
        lax.fori_loop(0, r, body, 0)
        fold(*at(2 * r), held_even)

    x_first(0)
    x_first(1)
    for i in range(CHUNKS + 4):
        if i < CHUNKS:
            x_second(i)
            if i + 2 < CHUNKS:
                x_first(i + 2)
        if 0 <= i - 1 < CHUNKS:
            select(i - 1)
            spread(i - 1)
        if 0 <= i - 2 < CHUNKS:
            pass_keys(i - 2)
        if 0 <= i - 3 < CHUNKS:
            pass_again(i - 3)
        if 0 <= i - 4 < CHUNKS:
            first_pass(i - 4)

    for kj in range(CHUNKS):
        top = jnp.max(col_top[kj], axis=0, keepdims=True)
        total = jnp.sum(col_sum[kj] * jnp.exp2(col_top[kj] - top), axis=0, keepdims=True)
        col_log[member, kj] = top + jnp.log2(total)
    team = [(1, sibling), (2, beside), (3, diagonal)]

    def mate(e):
        dh, dc = e // 2, e % 2
        return (1 - parity if dh else parity) * 2 + (1 - c if dc else c)

    for e, device in team:
        go(remote(col_log.at[member], col_log.at[member], cs.at[e], cr.at[e], device))

    lane = lax.broadcasted_iota(jnp.int32, (128, 128), 1)
    row_cols = jnp.zeros((128, 128), jnp.float32)
    for qi in range(CHUNKS):
        top = jnp.max(row_top[qi], axis=1, keepdims=True)
        total = jnp.sum(row_sum[qi] * jnp.exp2(row_top[qi] - top), axis=1, keepdims=True)
        row_cols = jnp.where(lane == qi, top + jnp.log2(total), row_cols)
    row_log = jnp.transpose(row_cols)[:8]

    for e, _ in team:
        landed(col_log.at[mate(e)], cs.at[e], cr.at[e])
    cols = []
    for kj in range(CHUNKS):
        logs = [col_log[m, kj] for m in range(MEMBERS)]
        top = jnp.maximum(jnp.maximum(logs[0], logs[1]), jnp.maximum(logs[2], logs[3]))
        total = sum(jnp.exp2(v - top) for v in logs)
        full = top + jnp.log2(total)
        col_half[kj] = full * 0.5
        mine = full[:, :128]
        for m in range(1, MEMBERS):
            mine = jnp.where(member == m, full[:, m * 128 : (m + 1) * 128], mine)
        cols.append(mine)
    own_col = jnp.concatenate(cols, axis=0)

    def second(qi, carry):
        best = [None] * 8
        for kj in range(CHUNKS):
            half_log = col_half[kj]
            for g in range(8):
                t = scores[qi, kj, pl.ds(g * 16, 16), :]
                t = t - half_log
                parts = [t[:, m * 128 : (m + 1) * 128] for m in range(MEMBERS)]
                part = jnp.maximum(
                    jnp.maximum(parts[0], parts[1]), jnp.maximum(parts[2], parts[3])
                )
                best[g] = part if kj == 0 else jnp.maximum(best[g], part)
        for g in range(8):
            rows = pl.ds(g * 16, 16)
            most = jnp.max(best[g], axis=1, keepdims=True)
            best_cols[rows, :] = jnp.where(lane[:16] == qi, most, best_cols[rows, :])
        return carry

    best_cols[...] = jnp.zeros((128, 128), jnp.float32)
    lax.fori_loop(0, CHUNKS, second, 0)
    best = 2.0 * jnp.transpose(best_cols[...])[:8] - row_log

    chunk = lax.broadcasted_iota(jnp.int32, (8, 128), 0)
    lane8 = lax.broadcasted_iota(jnp.int32, (8, 128), 1)
    index = slot_index(z, c, chunk, lane8)
    query_valid = index < query_count
    results = (
        jnp.where(query_valid, row_log * LN2, 0.0),
        jnp.where(index < key_count, own_col * LN2, 0.0),
        jnp.where(query_valid, best * LN2, 0.0),
    )
    for j, value in enumerate(results):
        value = block_transpose(value)
        for s in range(SOURCES):
            sent[s, pl.ds(j, 1), :] = value[s : s + 1]
    for dy in range(4):
        for dk in range(2):
            e = dy * 2 + dk
            to = peer_place(dy, dk)
            if e == 0:
                pltpu.make_async_copy(sent.at[to], got.at[place], or_.at[place]).start()
            else:
                go(remote(sent.at[to], got.at[place], os_.at[e], or_.at[place], peer(dy, dk)))
    for s in range(SOURCES):
        landed(got.at[s], os_.at[0], or_.at[s])
    for s in range(SOURCES):
        for j in range(3):
            out[j, pl.ds(s, 1), :] = got[s, pl.ds(j, 1), :]
    for copy in started:
        copy.wait_send()


def local(descriptors, pairs, counts):
    scale = 2.0 / math.sqrt(descriptors.shape[2]) * LOG2E
    width = descriptors.shape[2]
    bf16, f32 = jnp.bfloat16, jnp.float32
    dma = pltpu.SemaphoreType.DMA
    scratch = [pltpu.VMEM((GROUPS * IMAGES, ROWS, width), bf16) for _ in range(CHUNKS)]
    scratch += [pltpu.VMEM((8, 2, ROWS, width), bf16) for _ in range(CHUNKS)]
    scratch += [
        pltpu.VMEM((CHUNKS, SOURCES, ROWS, width), bf16),
        pltpu.VMEM((CHUNKS, MEMBERS, SOURCES, ROWS, width), bf16),
        pltpu.VMEM((CHUNKS, CHUNKS, 128, 512), f32),
        pltpu.VMEM((CHUNKS, 128, 128), f32),
        pltpu.VMEM((CHUNKS, 128, 128), f32),
        pltpu.VMEM((CHUNKS, 8, 512), f32),
        pltpu.VMEM((CHUNKS, 8, 512), f32),
        pltpu.VMEM((CHUNKS, 1, 512), f32),
        pltpu.VMEM((CHUNKS, 128, 128), f32),
        pltpu.VMEM((MEMBERS, CHUNKS, 1, 512), f32),
        pltpu.VMEM((CHUNKS, 1, 512), f32),
        pltpu.VMEM((128, 128), f32),
        pltpu.VMEM((128, 512), f32),
        pltpu.VMEM((128, 512), f32),
        pltpu.VMEM((8, 8, 128), f32),
        pltpu.VMEM((8, 8, 128), f32),
        dma((CHUNKS,)),
        dma((4, CHUNKS)), dma((4, CHUNKS)),
        dma((CHUNKS, 8)), dma((CHUNKS, 8)),
        dma((CHUNKS, 8)), dma((CHUNKS, 8)),
        dma((3, CHUNKS)), dma((3, CHUNKS)),
        dma((4,)), dma((4,)),
        dma((8,)), dma((8,)),
    ]
    out = pl.pallas_call(
        functools.partial(kernel, scale),
        out_shape=jax.ShapeDtypeStruct((3, 8, 128), f32),
        in_specs=[
            pl.BlockSpec(memory_space=pltpu.SMEM),
            pl.BlockSpec(memory_space=pltpu.SMEM),
            pl.BlockSpec(memory_space=pl.ANY),
        ],
        out_specs=pl.BlockSpec(memory_space=pltpu.VMEM),
        scratch_shapes=scratch,
        compiler_params=pltpu.CompilerParams(
            collective_id=0, has_side_effects=True, vmem_limit_bytes=63 * 1024 * 1024
        ),
    )(pairs.T, counts, descriptors)
    return out[0], out[1], out[2]


def solution(mesh):
    torus = Mesh(
        mesh.devices.reshape(mesh.shape["grp"], 4, 4, 2), ("grp", "tile_0", "tile_1", "tile_2")
    )
    return jax.shard_map(
        local,
        mesh=torus,
        in_specs=(P("grp", TILE, None), P("grp", None), P()),
        out_specs=(P("grp", TILE), P("grp", TILE), P("grp", TILE)),
        check_vma=False,
    )
```

```python
import functools
import math

import jax
import jax.numpy as jnp
from jax import lax
from jax.experimental import pallas as pl
from jax.experimental.pallas import tpu as pltpu
from jax.sharding import Mesh
from jax.sharding import PartitionSpec as P

TILE = ("tile_0", "tile_1", "tile_2")
MESH = pl.DeviceIdType.MESH

NEGATIVE = -1e30
CHUNKS = 8
ROWS = 16
GROUPS = 4
IMAGES = 16
SOURCES = 8
MEMBERS = 4
ENTER = 10
RELAY = 5
WIDE = 1
LOG2E = math.log2(math.e)
LN2 = math.log(2.0)


def slot_index(z, core, chunk, lane):
    outer = jnp.logical_or(z == 0, z == 3)
    low = jnp.where(outer, 0, 1)
    high = jnp.where(outer, 3, 2)
    source = lane // ROWS
    z_source = jnp.where(source % 2 == 0, low, high)
    tile = (source // 2) * 8 + z_source * 2 + core
    return tile * (CHUNKS * ROWS) + chunk * ROWS + lane % ROWS


def block_transpose(x):
    sub = lax.broadcasted_iota(jnp.int32, (8, 128), 0)
    block = lax.broadcasted_iota(jnp.int32, (8, 128), 1) // ROWS
    out = x
    for d in range(8):
        moved = x if d == 0 else pltpu.roll(pltpu.roll(x, ROWS * d, 1), 8 - d, 0)
        out = jnp.where(block == (sub + d) % 8, moved, out)
    return out


def route(pairs, group, x):
    slots = []
    for pair in range(8):
        for side in range(2):
            image = pairs[group, side, pair]
            slots.append((lax.rem(image // IMAGES - group + GROUPS, GROUPS), lax.rem(image, IMAGES)))
    one = [[jnp.where(d == k, 1, 0) for d, _ in slots] for k in range(GROUPS)]
    near, far, behind = (sum(one[k]) for k in (1, 2, 3))
    least = jnp.maximum(jnp.maximum(far - RELAY, behind + far - ENTER), 0)
    most = jnp.minimum(jnp.minimum(far, RELAY), ENTER - near)
    by_right = jnp.minimum(jnp.maximum((behind + far - near + 1) // 2, least), most)
    rank = [0] * GROUPS
    routed = []
    for s, (d, image) in enumerate(slots):
        relay_left = rank[2] - by_right
        by_left = jnp.logical_or(d == 3, jnp.logical_and(d == 2, relay_left >= 0))
        from_right = jnp.logical_or(d == 1, jnp.logical_and(d == 2, relay_left < 0))
        right_place = jnp.where(d == 1, rank[1], near + rank[2])
        left_place = jnp.where(d == 3, rank[3], behind + relay_left)
        routed.append(
            (
                d, image,
                jnp.where(from_right, right_place, -1), jnp.where(by_left, left_place, -1),
                jnp.where(jnp.logical_and(d == 2, relay_left < 0), rank[2], -1),
                jnp.where(jnp.logical_and(d == 2, relay_left >= 0), relay_left, -1),
            )
        )
        for k in range(1, GROUPS):
            rank[k] = rank[k] + one[k][s]
    return routed, jnp.where(least > most, 1, 0)


def at_place(entries, k):
    return sum(jnp.where(place == k, value, 0) for place, value in entries)


def within(value, count):
    return jnp.minimum(jnp.maximum(value, 0), count - 1)


def kernel(scale, narrow, pairs, counts, desc, out, *scratch):
    if narrow:
        misfit, scratch = scratch[0], scratch[1:]
        every_pair, relay_code, enter_code, slot_code = scratch[-4:]
        middle, arrived, packed_middle, packed_arrived = (
            scratch[-4 - (4 - k) * CHUNKS : -4 - (3 - k) * CHUNKS] for k in range(4)
        )
        ps, pr = scratch[-4 - 4 * CHUNKS - 2 : -4 - 4 * CHUNKS]
        scratch = scratch[: -4 - 4 * CHUNKS - 2]

    def wide(r):
        return not narrow or r < WIDE

    gathered = scratch[:CHUNKS]
    staged = scratch[CHUNKS : 2 * CHUNKS]
    (
        queries, keys, scores, row_top, row_sum, col_top, col_sum, key_bias, query_bias,
        col_log, col_half, best_cols, held_even, held_odd, sent, got,
        load_sem, xs, xr, qs, qr, ks, kr, fs, fr, cs, cr, os_, or_,
    ) = scratch[2 * CHUNKS :]
    x, y, z, c = (lax.axis_index(a) for a in ("grp",) + TILE)
    right = (lax.rem(x + 1, 4), y, z, c)
    left = (lax.rem(x + 3, 4), y, z, c)
    half = z // 2
    parity = z % 2
    place = y * 2 + half
    member = parity * 2 + c
    z_beside = half * 2 + (1 - parity)
    beside = (x, y, z_beside, c)
    sibling = (x, y, z, 1 - c)
    opposite = (lax.rem(x + 2, 4), y, z, c)
    diagonal = (x, y, z_beside, 1 - c)
    member_beside = (1 - parity) * 2 + c

    def peer(dy, dk):
        return (x, lax.rem(y + dy, 4), z if dk == 0 else 3 - z, c)

    def peer_place(dy, dk):
        return lax.rem(y + dy, 4) * 2 + (half if dk == 0 else 1 - half)

    loads = [
        pltpu.make_async_copy(
            desc.at[:, pl.ds(r * ROWS, ROWS), :], gathered[r].at[pl.ds(0, IMAGES)], load_sem.at[r]
        )
        for r in range(CHUNKS)
    ]
    for load in loads:
        load.start()

    others = [(dy, dk) for dy in range(4) for dk in range(2) if (dy, dk) != (0, 0)]
    barrier = pltpu.get_barrier_semaphore()
    greeted = [right, left, beside, sibling, diagonal] + [peer(dy, dk) for dy, dk in others]
    if narrow:
        greeted.append(opposite)
    for device in greeted:
        pl.semaphore_signal(barrier, inc=1, device_id=device, device_id_type=MESH)

    p = place
    query_count = counts[pairs[0, p]]
    key_count = counts[pairs[1, p]]
    row_top[...] = jnp.full(row_top.shape, NEGATIVE, jnp.float32)
    row_sum[...] = jnp.zeros(row_sum.shape, jnp.float32)
    col_top[...] = jnp.full(col_top.shape, NEGATIVE, jnp.float32)
    col_sum[...] = jnp.zeros(col_sum.shape, jnp.float32)
    for r in range(CHUNKS):
        lane = lax.broadcasted_iota(jnp.int32, (1, 128), 1)
        for m in range(MEMBERS):
            index = slot_index(half * 2 + m // 2, m % 2, r, lane)
            key_bias[r, :, pl.ds(m * 128, 128)] = jnp.where(index < key_count, 0.0, NEGATIVE)
        sub = lax.broadcasted_iota(jnp.int32, (128, 128), 0)
        query_bias[r] = jnp.where(slot_index(z, c, r, sub) < query_count, 0.0, NEGATIVE)

    pl.semaphore_wait(barrier, len(greeted))

    def remote(src, dst, send, recv, device):
        return pltpu.make_async_remote_copy(
            src_ref=src, dst_ref=dst, send_sem=send, recv_sem=recv,
            device_id=device, device_id_type=MESH,
        )

    started = []

    def go(copy):
        copy.start()
        started.append(copy)

    def own(r):
        return gathered[r].at[pl.ds(0, IMAGES)]

    from_left = lambda r: gathered[r].at[pl.ds(16, 16)]
    from_right = lambda r: gathered[r].at[pl.ds(48, 16)]
    far_low = lambda r: gathered[r].at[pl.ds(32, 8)]
    far_high = lambda r: gathered[r].at[pl.ds(40, 8)]

    def x_first(r):
        loads[r].wait()
        if not wide(r):
            for k in range(2 * RELAY):
                packed_middle[r][k] = gathered[r][relay_code[k]]
            for k, device in ((0, left), (1, right)):
                part = pl.ds(k * RELAY, RELAY)
                go(remote(
                    packed_middle[r].at[part], middle[r].at[part], xs.at[k, r], xr.at[k, r], device
                ))
            return
        go(remote(own(r), from_left(r), xs.at[0, r], xr.at[0, r], right))
        go(remote(own(r), from_right(r), xs.at[1, r], xr.at[1, r], left))

    def landed(ref, send, recv):
        remote(ref, ref, send, recv, right).wait_recv()

    def choose(code, first, other):
        a = first[jnp.minimum(code, IMAGES - 1)]
        b = other[jnp.maximum(code - IMAGES, 0)]
        return lax.select(code < IMAGES, a, b)

    def x_second(r):
        if not wide(r):
            for k in range(2):
                landed(middle[r].at[pl.ds(k * RELAY, RELAY)], xs.at[k, r], xr.at[k, r])
            for k, device in ((0, left), (1, right)):
                for n in range(k * ENTER, (k + 1) * ENTER):
                    packed_arrived[r][n] = choose(enter_code[n], gathered[r], middle[r])
                part = pl.ds(k * ENTER, ENTER)
                go(remote(
                    packed_arrived[r].at[part], arrived[r].at[part],
                    xs.at[2 + k, r], xr.at[2 + k, r], device,
                ))
            return
        landed(from_left(r), xs.at[0, r], xr.at[0, r])
        go(remote(gathered[r].at[pl.ds(16, 8)], far_low(r), xs.at[2, r], xr.at[2, r], right))
        landed(from_right(r), xs.at[1, r], xr.at[1, r])
        go(remote(gathered[r].at[pl.ds(56, 8)], far_high(r), xs.at[3, r], xr.at[3, r], left))

    def select(r):
        if not wide(r):
            for k in range(2):
                landed(arrived[r].at[pl.ds(k * ENTER, ENTER)], xs.at[2 + k, r], xr.at[2 + k, r])
            for pair in range(8):
                for side in range(2):
                    code = slot_code[pair * 2 + side]
                    staged[r][pair, side] = choose(code, gathered[r], arrived[r])
            return
        landed(far_low(r), xs.at[2, r], xr.at[2, r])
        landed(far_high(r), xs.at[3, r], xr.at[3, r])
        for pair in range(8):
            for side in range(2):
                image = pairs[side, pair]
                turn = lax.rem(x + 4 - image // IMAGES, 4)
                staged[r][pair, side] = gathered[r][turn * IMAGES + image % IMAGES]

    def spread(r):
        for dy in range(4):
            for dk in range(2):
                to = peer_place(dy, dk)
                e = dy * 2 + dk
                z_to = z if dk == 0 else 3 - z
                m_to = (z_to % 2) * 2 + c
                q_src, k_src = staged[r].at[to, 0], staged[r].at[to, 1]
                q_dst, k_dst = queries.at[r, place], keys.at[r, m_to, place]
                if e == 0:
                    for copy in (
                        pltpu.make_async_copy(q_src, q_dst, qr.at[r, place]),
                        pltpu.make_async_copy(k_src, k_dst, kr.at[r, place]),
                    ):
                        copy.start()
                else:
                    go(remote(k_src, k_dst, ks.at[r, e], kr.at[r, place], peer(dy, dk)))
                    go(remote(q_src, q_dst, qs.at[r, e], qr.at[r, place], peer(dy, dk)))

    def pass_keys(r):
        for s in range(SOURCES):
            landed(keys.at[r, member, s], ks.at[r, 0], kr.at[r, s])
        block = keys.at[r, member]
        go(remote(block, block, fs.at[0, r], fr.at[0, r], beside))
        go(remote(block, block, fs.at[1, r], fr.at[1, r], sibling))

    def pass_again(r):
        block = keys.at[r, member_beside]
        landed(block, fs.at[0, r], fr.at[0, r])
        go(remote(block, block, fs.at[2, r], fr.at[2, r], sibling))

    def product(qi, kj, held):
        q = queries[qi].reshape(128, 256)
        k = keys[kj].reshape(512, 256)
        held[...] = lax.dot_general(
            q, k, (((1,), (1,)), ((), ())), preferred_element_type=jnp.float32
        )

    def fold(qi, kj, held):
        kb = key_bias[kj]
        top = col_top[kj]
        tops = []
        high = top
        for g in range(8):
            rows = pl.ds(g * 16, 16)
            t = held[rows, :] * scale + kb
            qb = query_bias[qi, rows, :]
            parts = [t[:, i * 128 : (i + 1) * 128] + qb for i in range(4)]
            tops.append(
                jnp.maximum(jnp.maximum(parts[0], parts[1]), jnp.maximum(parts[2], parts[3]))
            )
            both = jnp.concatenate(parts, axis=1)
            scores[qi, kj, rows, :] = both
            held[rows, :] = both
            high = jnp.maximum(high, jnp.maximum(both[:8], both[8:]))
        total = col_sum[kj] * jnp.exp2(top - high)
        for g in range(8):
            rows = pl.ds(g * 16, 16)
            t = held[rows, :]
            before = row_top[qi, rows, :]
            now = jnp.maximum(before, tops[g])
            acc = row_sum[qi, rows, :] * jnp.exp2(before - now)
            for i in range(4):
                acc += jnp.exp2(t[:, i * 128 : (i + 1) * 128] - now)
            row_sum[qi, rows, :] = acc
            row_top[qi, rows, :] = now
            total += jnp.exp2(t[:8] - high) + jnp.exp2(t[8:] - high)
        col_sum[kj] = total
        col_top[kj] = high

    def first_pass(r):
        for s in range(SOURCES):
            landed(queries.at[r, s], qs.at[r, 0], qr.at[r, s])
        landed(keys.at[r, parity * 2 + 1 - c], fs.at[1, r], fr.at[1, r])
        landed(keys.at[r, (1 - parity) * 2 + 1 - c], fs.at[2, r], fr.at[2, r])

        def at(n):
            return jnp.minimum(n, r), jnp.where(n <= r, r, n - r - 1)

        def body(n, carry):
            product(*at(2 * n + 1), held_odd)
            fold(*at(2 * n), held_even)
            product(*at(2 * n + 2), held_even)
            fold(*at(2 * n + 1), held_odd)
            return carry

        product(*at(0), held_even)
        lax.fori_loop(0, r, body, 0)
        fold(*at(2 * r), held_even)

    def work_out_routes():
        for side in range(2):
            for pair in range(8):
                every_pair[x, side, pair] = pairs[side, pair]
        for e in range(1, GROUPS):
            other = lax.rem(x + e, GROUPS)
            landed(every_pair.at[other], ps.at[e], pr.at[e])
        before, after, across = (lax.rem(x + k, GROUPS) for k in (3, 1, 2))
        routed, bad = route(every_pair, x, x)
        for s, (d, image, right_place, left_place, _, _) in enumerate(routed):
            far = jnp.where(
                right_place >= 0, within(right_place, ENTER), ENTER + within(left_place, ENTER)
            )
            slot_code[s] = jnp.where(d == 0, image, IMAGES + far)
        routed, now = route(every_pair, before, x)
        bad += now
        entries = [
            (p, jnp.where(d == 1, i, IMAGES + within(m, RELAY))) for d, i, p, _, m, _ in routed
        ]
        for k in range(ENTER):
            enter_code[k] = at_place(entries, k)
        routed, now = route(every_pair, after, x)
        bad += now
        entries = [
            (p, jnp.where(d == 3, i, IMAGES + RELAY + within(m, RELAY)))
            for d, i, _, p, _, m in routed
        ]
        for k in range(ENTER):
            enter_code[ENTER + k] = at_place(entries, k)
        routed, now = route(every_pair, across, x)
        bad += now
        for k in range(RELAY):
            relay_code[k] = at_place([(m, i) for _, i, _, _, m, _ in routed], k)
            relay_code[RELAY + k] = at_place([(m, i) for _, i, _, _, _, m in routed], k)
        misfit[...] = jnp.full(misfit.shape, bad, jnp.int32)

    if narrow:
        for e, device in ((3, right), (1, left), (2, opposite)):
            go(remote(pairs, every_pair.at[x], ps.at[e], pr.at[e], device))
    x_first(0)
    if narrow:
        work_out_routes()
    x_first(1)
    for i in range(CHUNKS + 4):
        if i < CHUNKS:
            x_second(i)
            if i + 2 < CHUNKS:
                x_first(i + 2)
        if 0 <= i - 1 < CHUNKS:
            select(i - 1)
            spread(i - 1)
        if 0 <= i - 2 < CHUNKS:
            pass_keys(i - 2)
        if 0 <= i - 3 < CHUNKS:
            pass_again(i - 3)
        if 0 <= i - 4 < CHUNKS:
            first_pass(i - 4)

    for kj in range(CHUNKS):
        top = jnp.max(col_top[kj], axis=0, keepdims=True)
        total = jnp.sum(col_sum[kj] * jnp.exp2(col_top[kj] - top), axis=0, keepdims=True)
        col_log[member, kj] = top + jnp.log2(total)
    team = [(1, sibling), (2, beside), (3, diagonal)]

    def mate(e):
        dh, dc = e // 2, e % 2
        return (1 - parity if dh else parity) * 2 + (1 - c if dc else c)

    for e, device in team:
        go(remote(col_log.at[member], col_log.at[member], cs.at[e], cr.at[e], device))

    lane = lax.broadcasted_iota(jnp.int32, (128, 128), 1)
    row_cols = jnp.zeros((128, 128), jnp.float32)
    for qi in range(CHUNKS):
        top = jnp.max(row_top[qi], axis=1, keepdims=True)
        total = jnp.sum(row_sum[qi] * jnp.exp2(row_top[qi] - top), axis=1, keepdims=True)
        row_cols = jnp.where(lane == qi, top + jnp.log2(total), row_cols)
    row_log = jnp.transpose(row_cols)[:8]

    for e, _ in team:
        landed(col_log.at[mate(e)], cs.at[e], cr.at[e])
    cols = []
    for kj in range(CHUNKS):
        logs = [col_log[m, kj] for m in range(MEMBERS)]
        top = jnp.maximum(jnp.maximum(logs[0], logs[1]), jnp.maximum(logs[2], logs[3]))
        total = sum(jnp.exp2(v - top) for v in logs)
        full = top + jnp.log2(total)
        col_half[kj] = full * 0.5
        mine = full[:, :128]
        for m in range(1, MEMBERS):
            mine = jnp.where(member == m, full[:, m * 128 : (m + 1) * 128], mine)
        cols.append(mine)
    own_col = jnp.concatenate(cols, axis=0)

    def second(qi, carry):
        best = [None] * 8
        for kj in range(CHUNKS):
            half_log = col_half[kj]
            for g in range(8):
                t = scores[qi, kj, pl.ds(g * 16, 16), :]
                t = t - half_log
                parts = [t[:, m * 128 : (m + 1) * 128] for m in range(MEMBERS)]
                part = jnp.maximum(
                    jnp.maximum(parts[0], parts[1]), jnp.maximum(parts[2], parts[3])
                )
                best[g] = part if kj == 0 else jnp.maximum(best[g], part)
        for g in range(8):
            rows = pl.ds(g * 16, 16)
            most = jnp.max(best[g], axis=1, keepdims=True)
            best_cols[rows, :] = jnp.where(lane[:16] == qi, most, best_cols[rows, :])
        return carry

    best_cols[...] = jnp.zeros((128, 128), jnp.float32)
    lax.fori_loop(0, CHUNKS, second, 0)
    best = 2.0 * jnp.transpose(best_cols[...])[:8] - row_log

    chunk = lax.broadcasted_iota(jnp.int32, (8, 128), 0)
    lane8 = lax.broadcasted_iota(jnp.int32, (8, 128), 1)
    index = slot_index(z, c, chunk, lane8)
    query_valid = index < query_count
    results = (
        jnp.where(query_valid, row_log * LN2, 0.0),
        jnp.where(index < key_count, own_col * LN2, 0.0),
        jnp.where(query_valid, best * LN2, 0.0),
    )
    for j, value in enumerate(results):
        value = block_transpose(value)
        for s in range(SOURCES):
            sent[s, pl.ds(j, 1), :] = value[s : s + 1]
    for dy in range(4):
        for dk in range(2):
            e = dy * 2 + dk
            to = peer_place(dy, dk)
            if e == 0:
                pltpu.make_async_copy(sent.at[to], got.at[place], or_.at[place]).start()
            else:
                go(remote(sent.at[to], got.at[place], os_.at[e], or_.at[place], peer(dy, dk)))
    for s in range(SOURCES):
        landed(got.at[s], os_.at[0], or_.at[s])
    for s in range(SOURCES):
        for j in range(3):
            out[j, pl.ds(s, 1), :] = got[s, pl.ds(j, 1), :]
    for copy in started:
        copy.wait_send()


def local(descriptors, pairs, counts):
    scale = 2.0 / math.sqrt(descriptors.shape[2]) * LOG2E
    width = descriptors.shape[2]
    bf16, f32 = jnp.bfloat16, jnp.float32
    dma = pltpu.SemaphoreType.DMA
    scratch = [pltpu.VMEM((GROUPS * IMAGES, ROWS, width), bf16) for _ in range(CHUNKS)]
    scratch += [pltpu.VMEM((8, 2, ROWS, width), bf16) for _ in range(CHUNKS)]
    scratch += [
        pltpu.VMEM((CHUNKS, SOURCES, ROWS, width), bf16),
        pltpu.VMEM((CHUNKS, MEMBERS, SOURCES, ROWS, width), bf16),
        pltpu.VMEM((CHUNKS, CHUNKS, 128, 512), f32),
        pltpu.VMEM((CHUNKS, 128, 128), f32),
        pltpu.VMEM((CHUNKS, 128, 128), f32),
        pltpu.VMEM((CHUNKS, 8, 512), f32),
        pltpu.VMEM((CHUNKS, 8, 512), f32),
        pltpu.VMEM((CHUNKS, 1, 512), f32),
        pltpu.VMEM((CHUNKS, 128, 128), f32),
        pltpu.VMEM((MEMBERS, CHUNKS, 1, 512), f32),
        pltpu.VMEM((CHUNKS, 1, 512), f32),
        pltpu.VMEM((128, 128), f32),
        pltpu.VMEM((128, 512), f32),
        pltpu.VMEM((128, 512), f32),
        pltpu.VMEM((8, 8, 128), f32),
        pltpu.VMEM((8, 8, 128), f32),
        dma((CHUNKS,)),
        dma((4, CHUNKS)), dma((4, CHUNKS)),
        dma((CHUNKS, 8)), dma((CHUNKS, 8)),
        dma((CHUNKS, 8)), dma((CHUNKS, 8)),
        dma((3, CHUNKS)), dma((3, CHUNKS)),
        dma((4,)), dma((4,)),
        dma((8,)), dma((8,)),
    ]
    smem, vmem = pltpu.SMEM, pltpu.VMEM

    def call(narrow):
        rooms = list(scratch)
        if narrow:
            rooms[WIDE:CHUNKS] = [vmem((IMAGES, ROWS, width), bf16)] * (CHUNKS - WIDE)
            rooms += [dma((GROUPS,)), dma((GROUPS,))]
            for room in (RELAY, ENTER, RELAY, ENTER):
                rooms += [vmem((2 * room, ROWS, width), bf16)] * CHUNKS
            rooms += [
                smem((GROUPS, 2, 8), jnp.int32),
                smem((2 * RELAY,), jnp.int32),
                smem((2 * ENTER,), jnp.int32),
                smem((IMAGES,), jnp.int32),
            ]
        shapes = [jax.ShapeDtypeStruct((3, 8, 128), f32), jax.ShapeDtypeStruct((8, 128), jnp.int32)]
        count = 2 if narrow else 1
        return pl.pallas_call(
            functools.partial(kernel, scale, narrow),
            out_shape=shapes[:count],
            in_specs=[
                pl.BlockSpec(memory_space=smem),
                pl.BlockSpec(memory_space=smem),
                pl.BlockSpec(memory_space=pl.ANY),
            ],
            out_specs=[pl.BlockSpec(memory_space=vmem)] * count,
            scratch_shapes=rooms,
            name="narrow" if narrow else "full",
            compiler_params=pltpu.CompilerParams(
                collective_id=1 if narrow else 0,
                has_side_effects=True,
                vmem_limit_bytes=63 * 1024 * 1024,
            ),
        )(pairs.T, counts, descriptors)

    def split(out):
        return out[0], out[1], out[2]

    out, misfit = call(True)
    return lax.cond(misfit[0, 0] > 0, lambda _: split(call(False)[0]), split, out)


def solution(mesh):
    torus = Mesh(
        mesh.devices.reshape(mesh.shape["grp"], 4, 4, 2), ("grp", "tile_0", "tile_1", "tile_2")
    )
    return jax.shard_map(
        local,
        mesh=torus,
        in_specs=(P("grp", TILE, None), P("grp", None), P()),
        out_specs=(P("grp", TILE), P("grp", TILE), P("grp", TILE)),
        check_vma=False,
    )
```

```python
import functools
import math

import jax
import jax.numpy as jnp
from jax import lax
from jax.experimental import pallas as pl
from jax.experimental.pallas import tpu as pltpu
from jax.sharding import Mesh
from jax.sharding import PartitionSpec as P

TILE = ("tile_0", "tile_1", "tile_2")
MESH = pl.DeviceIdType.MESH

NEGATIVE = -1e30
CHUNKS = 8
ROWS = 16
GROUPS = 4
IMAGES = 16
SOURCES = 8
MEMBERS = 4
ENTER = 9
RELAY = 4
WIDE = 1
ORDER = (
    ("first", 1), ("second", 0), ("first", 2), ("first", 3), ("second", 1), ("first", 4),
    ("spread", 0), ("second", 2), ("first", 5), ("second", 3), ("first", 6), ("spread", 1),
    ("second", 4), ("first", 7), ("spread", 2), ("second", 5), ("keys", 0), ("spread", 3),
    ("second", 6), ("keys", 1), ("spread", 4), ("second", 7), ("again", 0), ("keys", 2),
    ("spread", 5), ("fold", 0, 1), ("again", 1), ("spread", 6), ("keys", 3), ("fold", 1, 3),
    ("spread", 7), ("again", 2), ("keys", 4), ("fold", 2, 5), ("again", 3), ("keys", 5),
    ("fold", 3, 3), ("keys", 6), ("again", 4), ("fold", 3, 4), ("fold", 4, 3), ("keys", 7),
    ("again", 5), ("fold", 4, 6), ("fold", 5, 3), ("again", 6), ("fold", 5, 8), ("fold", 6, 3),
    ("again", 7), ("fold", 6, 10), ("fold", 7, 15),
)
LOG2E = math.log2(math.e)
LN2 = math.log(2.0)


def slot_index(z, core, chunk, lane):
    outer = jnp.logical_or(z == 0, z == 3)
    low = jnp.where(outer, 0, 1)
    high = jnp.where(outer, 3, 2)
    source = lane // ROWS
    z_source = jnp.where(source % 2 == 0, low, high)
    tile = (source // 2) * 8 + z_source * 2 + core
    return tile * (CHUNKS * ROWS) + chunk * ROWS + lane % ROWS


def block_transpose(x):
    sub = lax.broadcasted_iota(jnp.int32, (8, 128), 0)
    block = lax.broadcasted_iota(jnp.int32, (8, 128), 1) // ROWS
    out = x
    for d in range(8):
        moved = x if d == 0 else pltpu.roll(pltpu.roll(x, ROWS * d, 1), 8 - d, 0)
        out = jnp.where(block == (sub + d) % 8, moved, out)
    return out


def route(pairs, group):
    slots = []
    images = []
    for pair in range(8):
        for side in range(2):
            image = pairs[group, side, pair]
            away = lax.rem(image // IMAGES - group + GROUPS, GROUPS)
            for earlier in images:
                away = jnp.where(image == earlier, 0, away)
            images.append(image)
            slots.append((away, lax.rem(image, IMAGES)))
    one = [[jnp.where(d == k, 1, 0) for d, _ in slots] for k in range(GROUPS)]
    near, far, behind = (sum(one[k]) for k in (1, 2, 3))
    least = jnp.maximum(jnp.maximum(far - RELAY, behind + far - ENTER), 0)
    most = jnp.minimum(jnp.minimum(far, RELAY), ENTER - near)
    by_right = jnp.minimum(jnp.maximum((behind + far - near + 1) // 2, least), most)
    rank = [0] * GROUPS
    routed = []
    for s, (d, image) in enumerate(slots):
        relay_left = rank[2] - by_right
        by_left = jnp.logical_or(d == 3, jnp.logical_and(d == 2, relay_left >= 0))
        from_right = jnp.logical_or(d == 1, jnp.logical_and(d == 2, relay_left < 0))
        right_place = jnp.where(d == 1, rank[1], near + rank[2])
        left_place = jnp.where(d == 3, rank[3], behind + relay_left)
        routed.append(
            (
                d, image,
                jnp.where(from_right, right_place, -1), jnp.where(by_left, left_place, -1),
                jnp.where(jnp.logical_and(d == 2, relay_left < 0), rank[2], -1),
                jnp.where(jnp.logical_and(d == 2, relay_left >= 0), relay_left, -1),
            )
        )
        for k in range(1, GROUPS):
            rank[k] = rank[k] + one[k][s]
    return images, routed, jnp.where(least > most, 1, 0)


def at_place(entries, k):
    return sum(jnp.where(place == k, value, 0) for place, value in entries)


def within(value, count):
    return jnp.minimum(jnp.maximum(value, 0), count - 1)


def kernel(scale, narrow, pairs_in, counts_in, desc, out, *scratch):
    if narrow:
        misfit, scratch = scratch[0], scratch[1:]
        every_pair, relay_code, enter_code, slot_code = scratch[-4:]
        middle, arrived, packed_middle, packed_arrived = (
            scratch[-4 - (4 - k) * CHUNKS : -4 - (3 - k) * CHUNKS] for k in range(4)
        )
        ps, pr = scratch[-4 - 4 * CHUNKS - 2 : -4 - 4 * CHUNKS]
        scratch = scratch[: -4 - 4 * CHUNKS - 2]

    def wide(r):
        return not narrow or r < WIDE

    gathered = scratch[:CHUNKS]
    staged = scratch[CHUNKS : 2 * CHUNKS]
    (
        queries, keys, scores, row_top, row_sum, col_top, col_sum, key_bias, query_bias,
        col_log, col_half, best_cols, turned, held_even, held_odd, sent, got,
        load_sem, xs, xr, qs, qr, ks, kr, fs, fr, cs, cr, os_, or_,
        pairs, counts, small_sem,
    ) = scratch[2 * CHUNKS :]
    x, y, z, c = (lax.axis_index(a) for a in ("grp",) + TILE)
    right = (lax.rem(x + 1, 4), y, z, c)
    left = (lax.rem(x + 3, 4), y, z, c)
    half = z // 2
    parity = z % 2
    place = y * 2 + half
    member = parity * 2 + c
    z_beside = half * 2 + (1 - parity)
    beside = (x, y, z_beside, c)
    sibling = (x, y, z, 1 - c)
    opposite = (lax.rem(x + 2, 4), y, z, c)
    diagonal = (x, y, z_beside, 1 - c)
    member_beside = (1 - parity) * 2 + c

    def peer(dy, dk):
        return (x, lax.rem(y + dy, 4), z if dk == 0 else 3 - z, c)

    def peer_place(dy, dk):
        return lax.rem(y + dy, 4) * 2 + (half if dk == 0 else 1 - half)

    others = [(dy, dk) for dy in range(4) for dk in range(2) if (dy, dk) != (0, 0)]
    barrier = pltpu.get_barrier_semaphore()
    greeted = [right, left, beside, sibling, diagonal] + [peer(dy, dk) for dy, dk in others]
    if narrow:
        greeted.append(opposite)
    for device in greeted:
        pl.semaphore_signal(barrier, inc=1, device_id=device, device_id_type=MESH)

    small = [
        pltpu.make_async_copy(pairs_in, pairs, small_sem.at[0]),
        pltpu.make_async_copy(counts_in, counts, small_sem.at[1]),
    ]
    for copy in small:
        copy.start()
    loads = [
        pltpu.make_async_copy(
            desc.at[:, pl.ds(r * ROWS, ROWS), :], gathered[r].at[pl.ds(0, IMAGES)], load_sem.at[r]
        )
        for r in range(CHUNKS)
    ]
    for load in loads:
        load.start()

    for copy in small:
        copy.wait()
    p = place
    query_count = counts[pairs[0, p]]
    key_count = counts[pairs[1, p]]
    row_top[...] = jnp.full(row_top.shape, NEGATIVE, jnp.float32)
    row_sum[...] = jnp.zeros(row_sum.shape, jnp.float32)
    col_top[...] = jnp.full(col_top.shape, NEGATIVE, jnp.float32)
    col_sum[...] = jnp.zeros(col_sum.shape, jnp.float32)
    for r in range(CHUNKS):
        lane = lax.broadcasted_iota(jnp.int32, (1, 128), 1)
        for m in range(MEMBERS):
            index = slot_index(half * 2 + m // 2, m % 2, r, lane)
            key_bias[r, :, pl.ds(m * 128, 128)] = jnp.where(index < key_count, 0.0, NEGATIVE)
        sub = lax.broadcasted_iota(jnp.int32, (128, 128), 0)
        query_bias[r] = jnp.where(slot_index(z, c, r, sub) < query_count, 0.0, NEGATIVE)

    pl.semaphore_wait(barrier, len(greeted))

    def remote(src, dst, send, recv, device):
        return pltpu.make_async_remote_copy(
            src_ref=src, dst_ref=dst, send_sem=send, recv_sem=recv,
            device_id=device, device_id_type=MESH,
        )

    started = []

    def go(copy):
        copy.start()
        started.append(copy)

    def own(r):
        return gathered[r].at[pl.ds(0, IMAGES)]

    from_left = lambda r: gathered[r].at[pl.ds(16, 16)]
    from_right = lambda r: gathered[r].at[pl.ds(48, 16)]
    far_low = lambda r: gathered[r].at[pl.ds(32, 8)]
    far_high = lambda r: gathered[r].at[pl.ds(40, 8)]

    def x_first(r):
        loads[r].wait()
        if not wide(r):
            for k in range(2 * RELAY):
                packed_middle[r][k] = gathered[r][relay_code[k]]
            for k, device in ((0, left), (1, right)):
                part = pl.ds(k * RELAY, RELAY)
                go(remote(
                    packed_middle[r].at[part], middle[r].at[part], xs.at[k, r], xr.at[k, r], device
                ))
            return
        go(remote(own(r), from_left(r), xs.at[0, r], xr.at[0, r], right))
        go(remote(own(r), from_right(r), xs.at[1, r], xr.at[1, r], left))

    def landed(ref, send, recv):
        remote(ref, ref, send, recv, right).wait_recv()

    def choose(code, first, other):
        a = first[jnp.minimum(code, IMAGES - 1)]
        b = other[jnp.maximum(code - IMAGES, 0)]
        return lax.select(code < IMAGES, a, b)

    def x_second(r):
        if not wide(r):
            for k in range(2):
                landed(middle[r].at[pl.ds(k * RELAY, RELAY)], xs.at[k, r], xr.at[k, r])
            for k, device in ((0, left), (1, right)):
                for n in range(k * ENTER, (k + 1) * ENTER):
                    packed_arrived[r][n] = choose(enter_code[n], gathered[r], middle[r])
                part = pl.ds(k * ENTER, ENTER)
                go(remote(
                    packed_arrived[r].at[part], arrived[r].at[part],
                    xs.at[2 + k, r], xr.at[2 + k, r], device,
                ))
            return
        landed(from_left(r), xs.at[0, r], xr.at[0, r])
        go(remote(gathered[r].at[pl.ds(16, 8)], far_low(r), xs.at[2, r], xr.at[2, r], right))
        landed(from_right(r), xs.at[1, r], xr.at[1, r])
        go(remote(gathered[r].at[pl.ds(56, 8)], far_high(r), xs.at[3, r], xr.at[3, r], left))

    def select(r):
        if not wide(r):
            for k in range(2):
                landed(arrived[r].at[pl.ds(k * ENTER, ENTER)], xs.at[2 + k, r], xr.at[2 + k, r])
            for pair in range(8):
                for side in range(2):
                    code = slot_code[pair * 2 + side]
                    staged[r][pair, side] = choose(code, gathered[r], arrived[r])
            return
        landed(far_low(r), xs.at[2, r], xr.at[2, r])
        landed(far_high(r), xs.at[3, r], xr.at[3, r])
        for pair in range(8):
            for side in range(2):
                image = pairs[side, pair]
                turn = lax.rem(x + 4 - image // IMAGES, 4)
                staged[r][pair, side] = gathered[r][turn * IMAGES + image % IMAGES]

    def spread(r):
        for dy in range(4):
            for dk in range(2):
                to = peer_place(dy, dk)
                e = dy * 2 + dk
                z_to = z if dk == 0 else 3 - z
                m_to = (z_to % 2) * 2 + c
                q_src, k_src = staged[r].at[to, 0], staged[r].at[to, 1]
                q_dst, k_dst = queries.at[r, place], keys.at[r, m_to, place]
                if e == 0:
                    for copy in (
                        pltpu.make_async_copy(q_src, q_dst, qr.at[r, place]),
                        pltpu.make_async_copy(k_src, k_dst, kr.at[r, place]),
                    ):
                        copy.start()
                else:
                    go(remote(k_src, k_dst, ks.at[r, e], kr.at[r, place], peer(dy, dk)))
                    go(remote(q_src, q_dst, qs.at[r, e], qr.at[r, place], peer(dy, dk)))

    def pass_keys(r):
        for s in range(SOURCES):
            landed(keys.at[r, member, s], ks.at[r, 0], kr.at[r, s])
        block = keys.at[r, member]
        go(remote(block, block, fs.at[0, r], fr.at[0, r], beside))
        go(remote(block, block, fs.at[1, r], fr.at[1, r], sibling))

    def pass_again(r):
        block = keys.at[r, member_beside]
        landed(block, fs.at[0, r], fr.at[0, r])
        go(remote(block, block, fs.at[2, r], fr.at[2, r], sibling))

    def product(qi, kj):
        q = queries[qi].reshape(128, 256)
        return jnp.dot(q, turned[kj], preferred_element_type=jnp.float32)

    def fold(qi, kj, held):
        kb = key_bias[kj]
        top = col_top[kj]
        high = top
        tops = []
        for g in range(8):
            rows = pl.ds(g * 16, 16)
            t = held[rows, :] * scale + kb
            qb = query_bias[qi, rows, :]
            parts = [t[:, i * 128 : (i + 1) * 128] + qb for i in range(4)]
            tops.append(
                jnp.maximum(jnp.maximum(parts[0], parts[1]), jnp.maximum(parts[2], parts[3]))
            )
            both = jnp.concatenate(parts, axis=1)
            scores[qi, kj, rows, :] = both
            high = jnp.maximum(high, jnp.maximum(both[:8], both[8:]))
        total = col_sum[kj] * jnp.exp2(top - high)
        for g in range(8):
            rows = pl.ds(g * 16, 16)
            t = scores[qi, kj, rows, :]
            before = row_top[qi, rows, :]
            now = jnp.maximum(before, tops[g])
            acc = row_sum[qi, rows, :] * jnp.exp2(before - now)
            for i in range(4):
                acc += jnp.exp2(t[:, i * 128 : (i + 1) * 128] - now)
            row_sum[qi, rows, :] = acc
            row_top[qi, rows, :] = now
            total += jnp.exp2(t[:8] - high) + jnp.exp2(t[8:] - high)
        col_sum[kj] = total
        col_top[kj] = high

    def fold_tiles(at, count):
        def ahead(n):
            return product(*at(jnp.minimum(n, count - 1)))

        def body(i, carry):
            now, then = ahead(2 * i + 2), ahead(2 * i + 3)
            fold(*at(2 * i), held_even)
            fold(*at(2 * i + 1), held_odd)
            held_even[...] = now
            held_odd[...] = then
            return carry

        held_even[...] = ahead(0)
        if count > 1:
            held_odd[...] = ahead(1)
            lax.fori_loop(0, count // 2, body, 0)
        if count % 2:
            fold(*at(count - 1), held_even)

    def wait_chunk(r):
        for s in range(SOURCES):
            landed(queries.at[r, s], qs.at[r, 0], qr.at[r, s])
        landed(keys.at[r, parity * 2 + 1 - c], fs.at[1, r], fr.at[1, r])
        landed(keys.at[r, (1 - parity) * 2 + 1 - c], fs.at[2, r], fr.at[2, r])
        turned[r] = jnp.transpose(keys[r].reshape(512, 256))

    def first_pass(r, begin, count):
        if begin == 0:
            wait_chunk(r)

        def at(n):
            n = n + begin
            return jnp.minimum(n, r), jnp.where(n <= r, r, n - r - 1)

        fold_tiles(at, count)

    def work_out_routes():
        for side in range(2):
            for pair in range(8):
                every_pair[x, side, pair] = pairs[side, pair]
        for e in range(1, GROUPS):
            other = lax.rem(x + e, GROUPS)
            landed(every_pair.at[other], ps.at[e], pr.at[e])
        before, after, across = (lax.rem(x + k, GROUPS) for k in (3, 1, 2))
        images, routed, bad = route(every_pair, x)
        codes = []
        for s, (d, image, right_place, left_place, _, _) in enumerate(routed):
            far = jnp.where(
                right_place >= 0, within(right_place, ENTER), ENTER + within(left_place, ENTER)
            )
            code = jnp.where(d == 0, image, IMAGES + far)
            for earlier, same in zip(images, codes):
                code = jnp.where(images[s] == earlier, same, code)
            codes.append(code)
            slot_code[s] = code
        _, routed, now = route(every_pair, before)
        bad += now
        entries = [
            (p, jnp.where(d == 1, i, IMAGES + within(m, RELAY))) for d, i, p, _, m, _ in routed
        ]
        for k in range(ENTER):
            enter_code[k] = at_place(entries, k)
        _, routed, now = route(every_pair, after)
        bad += now
        entries = [
            (p, jnp.where(d == 3, i, IMAGES + RELAY + within(m, RELAY)))
            for d, i, _, p, _, m in routed
        ]
        for k in range(ENTER):
            enter_code[ENTER + k] = at_place(entries, k)
        _, routed, now = route(every_pair, across)
        bad += now
        for k in range(RELAY):
            relay_code[k] = at_place([(m, i) for _, i, _, _, m, _ in routed], k)
            relay_code[RELAY + k] = at_place([(m, i) for _, i, _, _, _, m in routed], k)
        misfit[...] = jnp.full(misfit.shape, bad, jnp.int32)

    if narrow:
        for e, device in ((3, right), (1, left), (2, opposite)):
            go(remote(pairs, every_pair.at[x], ps.at[e], pr.at[e], device))
    x_first(0)
    if narrow:
        work_out_routes()
    taken = [0] * CHUNKS
    for step, r, *count in ORDER:
        if step == "first":
            x_first(r)
        elif step == "second":
            x_second(r)
        elif step == "spread":
            select(r)
            spread(r)
        elif step == "keys":
            pass_keys(r)
        elif step == "again":
            pass_again(r)
        elif narrow:
            first_pass(r, taken[r], count[0])
            taken[r] += count[0]
    if not narrow:
        for r in range(CHUNKS):
            wait_chunk(r)
        fold_tiles(lambda n: (n // CHUNKS, n % CHUNKS), CHUNKS * CHUNKS)

    for kj in range(CHUNKS):
        top = jnp.max(col_top[kj], axis=0, keepdims=True)
        total = jnp.sum(col_sum[kj] * jnp.exp2(col_top[kj] - top), axis=0, keepdims=True)
        col_log[member, kj] = top + jnp.log2(total)
    team = [(1, sibling), (2, beside), (3, diagonal)]

    def mate(e):
        dh, dc = e // 2, e % 2
        return (1 - parity if dh else parity) * 2 + (1 - c if dc else c)

    for e, device in team:
        go(remote(col_log.at[member], col_log.at[member], cs.at[e], cr.at[e], device))

    lane = lax.broadcasted_iota(jnp.int32, (128, 128), 1)
    row_cols = jnp.zeros((128, 128), jnp.float32)
    for qi in range(CHUNKS):
        top = jnp.max(row_top[qi], axis=1, keepdims=True)
        total = jnp.sum(row_sum[qi] * jnp.exp2(row_top[qi] - top), axis=1, keepdims=True)
        row_cols = jnp.where(lane == qi, top + jnp.log2(total), row_cols)
    row_log = jnp.transpose(row_cols)[:8]

    for e, _ in team:
        landed(col_log.at[mate(e)], cs.at[e], cr.at[e])
    cols = []
    for kj in range(CHUNKS):
        logs = [col_log[m, kj] for m in range(MEMBERS)]
        top = jnp.maximum(jnp.maximum(logs[0], logs[1]), jnp.maximum(logs[2], logs[3]))
        total = sum(jnp.exp2(v - top) for v in logs)
        full = top + jnp.log2(total)
        col_half[kj] = full * 0.5
        mine = full[:, :128]
        for m in range(1, MEMBERS):
            mine = jnp.where(member == m, full[:, m * 128 : (m + 1) * 128], mine)
        cols.append(mine)
    own_col = jnp.concatenate(cols, axis=0)

    def second(qi, carry):
        best = [None] * 8
        for kj in range(CHUNKS):
            half_log = col_half[kj]
            for g in range(8):
                t = scores[qi, kj, pl.ds(g * 16, 16), :]
                t = t - half_log
                parts = [t[:, m * 128 : (m + 1) * 128] for m in range(MEMBERS)]
                part = jnp.maximum(
                    jnp.maximum(parts[0], parts[1]), jnp.maximum(parts[2], parts[3])
                )
                best[g] = part if kj == 0 else jnp.maximum(best[g], part)
        for g in range(8):
            rows = pl.ds(g * 16, 16)
            most = jnp.max(best[g], axis=1, keepdims=True)
            best_cols[rows, :] = jnp.where(lane[:16] == qi, most, best_cols[rows, :])
        return carry

    best_cols[...] = jnp.zeros((128, 128), jnp.float32)
    lax.fori_loop(0, CHUNKS, second, 0)
    best = 2.0 * jnp.transpose(best_cols[...])[:8] - row_log

    chunk = lax.broadcasted_iota(jnp.int32, (8, 128), 0)
    lane8 = lax.broadcasted_iota(jnp.int32, (8, 128), 1)
    index = slot_index(z, c, chunk, lane8)
    query_valid = index < query_count
    results = (
        jnp.where(query_valid, row_log * LN2, 0.0),
        jnp.where(index < key_count, own_col * LN2, 0.0),
        jnp.where(query_valid, best * LN2, 0.0),
    )
    for j, value in enumerate(results):
        value = block_transpose(value)
        for s in range(SOURCES):
            sent[s, pl.ds(j, 1), :] = value[s : s + 1]
    for dy in range(4):
        for dk in range(2):
            e = dy * 2 + dk
            to = peer_place(dy, dk)
            if e == 0:
                pltpu.make_async_copy(sent.at[to], got.at[place], or_.at[place]).start()
            else:
                go(remote(sent.at[to], got.at[place], os_.at[e], or_.at[place], peer(dy, dk)))
    for s in range(SOURCES):
        landed(got.at[s], os_.at[0], or_.at[s])
    for s in range(SOURCES):
        for j in range(3):
            out[j, pl.ds(s, 1), :] = got[s, pl.ds(j, 1), :]
    for copy in started:
        copy.wait_send()


def local(descriptors, pairs, counts):
    scale = 2.0 / math.sqrt(descriptors.shape[2]) * LOG2E
    width = descriptors.shape[2]
    bf16, f32 = jnp.bfloat16, jnp.float32
    dma = pltpu.SemaphoreType.DMA
    scratch = [pltpu.VMEM((GROUPS * IMAGES, ROWS, width), bf16) for _ in range(CHUNKS)]
    scratch += [pltpu.VMEM((8, 2, ROWS, width), bf16) for _ in range(CHUNKS)]
    scratch += [
        pltpu.VMEM((CHUNKS, SOURCES, ROWS, width), bf16),
        pltpu.VMEM((CHUNKS, MEMBERS, SOURCES, ROWS, width), bf16),
        pltpu.VMEM((CHUNKS, CHUNKS, 128, 512), f32),
        pltpu.VMEM((CHUNKS, 128, 128), f32),
        pltpu.VMEM((CHUNKS, 128, 128), f32),
        pltpu.VMEM((CHUNKS, 8, 512), f32),
        pltpu.VMEM((CHUNKS, 8, 512), f32),
        pltpu.VMEM((CHUNKS, 1, 512), f32),
        pltpu.VMEM((CHUNKS, 128, 128), f32),
        pltpu.VMEM((MEMBERS, CHUNKS, 1, 512), f32),
        pltpu.VMEM((CHUNKS, 1, 512), f32),
        pltpu.VMEM((128, 128), f32),
        pltpu.VMEM((CHUNKS, width, 512), bf16),
        pltpu.VMEM((128, 512), f32),
        pltpu.VMEM((128, 512), f32),
        pltpu.VMEM((8, 8, 128), f32),
        pltpu.VMEM((8, 8, 128), f32),
        dma((CHUNKS,)),
        dma((4, CHUNKS)), dma((4, CHUNKS)),
        dma((CHUNKS, 8)), dma((CHUNKS, 8)),
        dma((CHUNKS, 8)), dma((CHUNKS, 8)),
        dma((3, CHUNKS)), dma((3, CHUNKS)),
        dma((4,)), dma((4,)),
        dma((8,)), dma((8,)),
        pltpu.SMEM((2, 8), jnp.int32), pltpu.SMEM((64,), jnp.int32), dma((2,)),
    ]
    smem, vmem = pltpu.SMEM, pltpu.VMEM

    def call(narrow):
        rooms = list(scratch)
        if narrow:
            rooms[WIDE:CHUNKS] = [vmem((IMAGES, ROWS, width), bf16)] * (CHUNKS - WIDE)
            rooms += [dma((GROUPS,)), dma((GROUPS,))]
            for room in (RELAY, ENTER, RELAY, ENTER):
                rooms += [vmem((2 * room, ROWS, width), bf16)] * CHUNKS
            rooms += [
                smem((GROUPS, 2, 8), jnp.int32),
                smem((2 * RELAY,), jnp.int32),
                smem((2 * ENTER,), jnp.int32),
                smem((IMAGES,), jnp.int32),
            ]
        shapes = [jax.ShapeDtypeStruct((3, 8, 128), f32), jax.ShapeDtypeStruct((8, 128), jnp.int32)]
        count = 2 if narrow else 1
        return pl.pallas_call(
            functools.partial(kernel, scale, narrow),
            out_shape=shapes[:count],
            in_specs=[
                pl.BlockSpec(memory_space=pl.ANY),
                pl.BlockSpec(memory_space=pl.ANY),
                pl.BlockSpec(memory_space=pl.ANY),
            ],
            out_specs=[pl.BlockSpec(memory_space=vmem)] * count,
            scratch_shapes=rooms,
            name="narrow" if narrow else "full",
            compiler_params=pltpu.CompilerParams(
                collective_id=1 if narrow else 0,
                has_side_effects=True,
                vmem_limit_bytes=63 * 1024 * 1024,
            ),
        )(pairs.T, counts, descriptors)

    def split(out):
        return out[0], out[1], out[2]

    out, misfit = call(True)
    return lax.cond(misfit[0, 0] > 0, lambda _: split(call(False)[0]), split, out)


def solution(mesh):
    torus = Mesh(
        mesh.devices.reshape(mesh.shape["grp"], 4, 4, 2), ("grp", "tile_0", "tile_1", "tile_2")
    )
    return jax.shard_map(
        local,
        mesh=torus,
        in_specs=(P("grp", TILE, None), P("grp", None), P()),
        out_specs=(P("grp", TILE), P("grp", TILE), P("grp", TILE)),
        check_vma=False,
    )
```

```python
import functools
import math

import jax
import jax.numpy as jnp
from jax import lax
from jax.experimental import pallas as pl
from jax.experimental.pallas import tpu as pltpu
from jax.sharding import Mesh
from jax.sharding import PartitionSpec as P

TILE = ("tile_0", "tile_1", "tile_2")
MESH = pl.DeviceIdType.MESH

NEGATIVE = -1e30
CHUNKS = 8
ROWS = 16
GROUPS = 4
IMAGES = 16
SOURCES = 8
MEMBERS = 4
ENTER = 9
RELAY = 4
WIDE = 2
ORDER = (
    ("second", 0), ("first", 2), ("first", 3), ("second", 1), ("first", 4), ("spread", 0),
    ("second", 2), ("first", 5), ("second", 3), ("first", 6), ("spread", 1), ("second", 4),
    ("first", 7), ("spread", 2), ("second", 5), ("keys", 0), ("spread", 3), ("second", 6),
    ("keys", 1), ("spread", 4), ("second", 7), ("again", 0), ("keys", 2), ("spread", 5),
    ("fold", 0, 1), ("spread", 6), ("keys", 3), ("again", 1), ("spread", 7), ("again", 2),
    ("keys", 4), ("fold", 1, 3), ("fold", 2, 2), ("again", 3), ("keys", 5), ("fold", 2, 3),
    ("fold", 3, 2), ("keys", 6), ("again", 4), ("fold", 3, 5), ("fold", 4, 2), ("keys", 7),
    ("again", 5), ("fold", 4, 7), ("fold", 5, 2), ("again", 6), ("fold", 5, 9), ("fold", 6, 2),
    ("again", 7), ("fold", 6, 11), ("fold", 7, 15),
)
LOG2E = math.log2(math.e)
LN2 = math.log(2.0)


def slot_index(z, core, chunk, lane):
    outer = jnp.logical_or(z == 0, z == 3)
    low = jnp.where(outer, 0, 1)
    high = jnp.where(outer, 3, 2)
    source = lane // ROWS
    z_source = jnp.where(source % 2 == 0, low, high)
    tile = (source // 2) * 8 + z_source * 2 + core
    return tile * (CHUNKS * ROWS) + chunk * ROWS + lane % ROWS


def block_transpose(x):
    sub = lax.broadcasted_iota(jnp.int32, (8, 128), 0)
    block = lax.broadcasted_iota(jnp.int32, (8, 128), 1) // ROWS
    out = x
    for d in range(8):
        moved = x if d == 0 else pltpu.roll(pltpu.roll(x, ROWS * d, 1), 8 - d, 0)
        out = jnp.where(block == (sub + d) % 8, moved, out)
    return out


def route(pairs, group):
    slots = []
    images = []
    for pair in range(8):
        for side in range(2):
            image = pairs[group, side, pair]
            away = lax.rem(image // IMAGES - group + GROUPS, GROUPS)
            for earlier in images:
                away = jnp.where(image == earlier, 0, away)
            images.append(image)
            slots.append((away, lax.rem(image, IMAGES)))
    one = [[jnp.where(d == k, 1, 0) for d, _ in slots] for k in range(GROUPS)]
    near, far, behind = (sum(one[k]) for k in (1, 2, 3))
    least = jnp.maximum(jnp.maximum(far - RELAY, behind + far - ENTER), 0)
    most = jnp.minimum(jnp.minimum(far, RELAY), ENTER - near)
    by_right = jnp.minimum(jnp.maximum((behind + far - near + 1) // 2, least), most)
    rank = [0] * GROUPS
    routed = []
    for s, (d, image) in enumerate(slots):
        relay_left = rank[2] - by_right
        by_left = jnp.logical_or(d == 3, jnp.logical_and(d == 2, relay_left >= 0))
        from_right = jnp.logical_or(d == 1, jnp.logical_and(d == 2, relay_left < 0))
        right_place = jnp.where(d == 1, rank[1], near + rank[2])
        left_place = jnp.where(d == 3, rank[3], behind + relay_left)
        routed.append(
            (
                d, image,
                jnp.where(from_right, right_place, -1), jnp.where(by_left, left_place, -1),
                jnp.where(jnp.logical_and(d == 2, relay_left < 0), rank[2], -1),
                jnp.where(jnp.logical_and(d == 2, relay_left >= 0), relay_left, -1),
            )
        )
        for k in range(1, GROUPS):
            rank[k] = rank[k] + one[k][s]
    return images, routed, jnp.where(least > most, 1, 0)


def at_place(entries, k):
    return sum(jnp.where(place == k, value, 0) for place, value in entries)


def within(value, count):
    return jnp.minimum(jnp.maximum(value, 0), count - 1)


def kernel(scale, narrow, pairs_in, counts_in, desc, out, *scratch):
    if narrow:
        misfit, scratch = scratch[0], scratch[1:]
        every_pair, relay_code, enter_code, slot_code = scratch[-4:]
        middle, arrived, packed_middle, packed_arrived = (
            scratch[-4 - (4 - k) * CHUNKS : -4 - (3 - k) * CHUNKS] for k in range(4)
        )
        ps, pr = scratch[-4 - 4 * CHUNKS - 2 : -4 - 4 * CHUNKS]
        scratch = scratch[: -4 - 4 * CHUNKS - 2]

    def wide(r):
        return not narrow or r < WIDE

    gathered = scratch[:CHUNKS]
    staged = scratch[CHUNKS : 2 * CHUNKS]
    (
        queries, keys, scores, row_top, row_sum, col_top, col_sum, key_bias, query_bias,
        col_log, col_half, best_cols, turned, held_even, held_odd, sent, got,
        load_sem, xs, xr, qs, qr, ks, kr, fs, fr, cs, cr, os_, or_,
        pairs, counts, small_sem,
    ) = scratch[2 * CHUNKS :]
    x, y, z, c = (lax.axis_index(a) for a in ("grp",) + TILE)
    right = (lax.rem(x + 1, 4), y, z, c)
    left = (lax.rem(x + 3, 4), y, z, c)
    half = z // 2
    parity = z % 2
    place = y * 2 + half
    member = parity * 2 + c
    z_beside = half * 2 + (1 - parity)
    beside = (x, y, z_beside, c)
    sibling = (x, y, z, 1 - c)
    opposite = (lax.rem(x + 2, 4), y, z, c)
    diagonal = (x, y, z_beside, 1 - c)
    member_beside = (1 - parity) * 2 + c

    def peer(dy, dk):
        return (x, lax.rem(y + dy, 4), z if dk == 0 else 3 - z, c)

    def peer_place(dy, dk):
        return lax.rem(y + dy, 4) * 2 + (half if dk == 0 else 1 - half)

    others = [(dy, dk) for dy in range(4) for dk in range(2) if (dy, dk) != (0, 0)]
    barrier = pltpu.get_barrier_semaphore()
    greeted = [right, left, beside, sibling, diagonal] + [peer(dy, dk) for dy, dk in others]
    if narrow:
        greeted.append(opposite)
    for device in greeted:
        pl.semaphore_signal(barrier, inc=1, device_id=device, device_id_type=MESH)

    small = [
        pltpu.make_async_copy(pairs_in, pairs, small_sem.at[0]),
        pltpu.make_async_copy(counts_in, counts, small_sem.at[1]),
    ]
    for copy in small:
        copy.start()
    loads = [
        pltpu.make_async_copy(
            desc.at[:, pl.ds(r * ROWS, ROWS), :], gathered[r].at[pl.ds(0, IMAGES)], load_sem.at[r]
        )
        for r in range(CHUNKS)
    ]
    for load in loads:
        load.start()

    for copy in small:
        copy.wait()
    p = place
    query_count = counts[pairs[0, p]]
    key_count = counts[pairs[1, p]]
    row_top[...] = jnp.full(row_top.shape, NEGATIVE, jnp.float32)
    row_sum[...] = jnp.zeros(row_sum.shape, jnp.float32)
    col_top[...] = jnp.full(col_top.shape, NEGATIVE, jnp.float32)
    col_sum[...] = jnp.zeros(col_sum.shape, jnp.float32)
    for r in range(CHUNKS):
        lane = lax.broadcasted_iota(jnp.int32, (1, 128), 1)
        for m in range(MEMBERS):
            index = slot_index(half * 2 + m // 2, m % 2, r, lane)
            key_bias[r, :, pl.ds(m * 128, 128)] = jnp.where(index < key_count, 0.0, NEGATIVE)
        sub = lax.broadcasted_iota(jnp.int32, (128, 128), 0)
        query_bias[r] = jnp.where(slot_index(z, c, r, sub) < query_count, 0.0, NEGATIVE)

    pl.semaphore_wait(barrier, len(greeted))

    def remote(src, dst, send, recv, device):
        return pltpu.make_async_remote_copy(
            src_ref=src, dst_ref=dst, send_sem=send, recv_sem=recv,
            device_id=device, device_id_type=MESH,
        )

    started = []

    def go(copy):
        copy.start()
        started.append(copy)

    def own(r):
        return gathered[r].at[pl.ds(0, IMAGES)]

    from_left = lambda r: gathered[r].at[pl.ds(16, 16)]
    from_right = lambda r: gathered[r].at[pl.ds(48, 16)]
    far_low = lambda r: gathered[r].at[pl.ds(32, 8)]
    far_high = lambda r: gathered[r].at[pl.ds(40, 8)]

    def x_first(r):
        loads[r].wait()
        if not wide(r):
            for k in range(2 * RELAY):
                packed_middle[r][k] = gathered[r][relay_code[k]]
            for k, device in ((0, left), (1, right)):
                part = pl.ds(k * RELAY, RELAY)
                go(remote(
                    packed_middle[r].at[part], middle[r].at[part], xs.at[k, r], xr.at[k, r], device
                ))
            return
        go(remote(own(r), from_left(r), xs.at[0, r], xr.at[0, r], right))
        go(remote(own(r), from_right(r), xs.at[1, r], xr.at[1, r], left))

    def landed(ref, send, recv):
        remote(ref, ref, send, recv, right).wait_recv()

    def choose(code, first, other):
        a = first[jnp.minimum(code, IMAGES - 1)]
        b = other[jnp.maximum(code - IMAGES, 0)]
        return lax.select(code < IMAGES, a, b)

    def x_second(r):
        if not wide(r):
            for k in range(2):
                landed(middle[r].at[pl.ds(k * RELAY, RELAY)], xs.at[k, r], xr.at[k, r])
            for k, device in ((0, left), (1, right)):
                for n in range(k * ENTER, (k + 1) * ENTER):
                    packed_arrived[r][n] = choose(enter_code[n], gathered[r], middle[r])
                part = pl.ds(k * ENTER, ENTER)
                go(remote(
                    packed_arrived[r].at[part], arrived[r].at[part],
                    xs.at[2 + k, r], xr.at[2 + k, r], device,
                ))
            return
        landed(from_left(r), xs.at[0, r], xr.at[0, r])
        go(remote(gathered[r].at[pl.ds(16, 8)], far_low(r), xs.at[2, r], xr.at[2, r], right))
        landed(from_right(r), xs.at[1, r], xr.at[1, r])
        go(remote(gathered[r].at[pl.ds(56, 8)], far_high(r), xs.at[3, r], xr.at[3, r], left))

    def select(r):
        if not wide(r):
            for k in range(2):
                landed(arrived[r].at[pl.ds(k * ENTER, ENTER)], xs.at[2 + k, r], xr.at[2 + k, r])
            for pair in range(8):
                for side in range(2):
                    code = slot_code[pair * 2 + side]
                    staged[r][pair, side] = choose(code, gathered[r], arrived[r])
            return
        landed(far_low(r), xs.at[2, r], xr.at[2, r])
        landed(far_high(r), xs.at[3, r], xr.at[3, r])
        for pair in range(8):
            for side in range(2):
                image = pairs[side, pair]
                turn = lax.rem(x + 4 - image // IMAGES, 4)
                staged[r][pair, side] = gathered[r][turn * IMAGES + image % IMAGES]

    def spread(r):
        for dy in range(4):
            for dk in range(2):
                to = peer_place(dy, dk)
                e = dy * 2 + dk
                z_to = z if dk == 0 else 3 - z
                m_to = (z_to % 2) * 2 + c
                q_src, k_src = staged[r].at[to, 0], staged[r].at[to, 1]
                q_dst, k_dst = queries.at[r, place], keys.at[r, m_to, place]
                if e == 0:
                    for copy in (
                        pltpu.make_async_copy(q_src, q_dst, qr.at[r, place]),
                        pltpu.make_async_copy(k_src, k_dst, kr.at[r, place]),
                    ):
                        copy.start()
                else:
                    go(remote(k_src, k_dst, ks.at[r, e], kr.at[r, place], peer(dy, dk)))
                    go(remote(q_src, q_dst, qs.at[r, e], qr.at[r, place], peer(dy, dk)))

    def pass_keys(r):
        for s in range(SOURCES):
            landed(keys.at[r, member, s], ks.at[r, 0], kr.at[r, s])
        block = keys.at[r, member]
        go(remote(block, block, fs.at[0, r], fr.at[0, r], beside))
        go(remote(block, block, fs.at[1, r], fr.at[1, r], sibling))

    def pass_again(r):
        block = keys.at[r, member_beside]
        landed(block, fs.at[0, r], fr.at[0, r])
        go(remote(block, block, fs.at[2, r], fr.at[2, r], sibling))

    def product(qi, kj):
        q = queries[qi].reshape(128, 256)
        return jnp.dot(q, turned[kj], preferred_element_type=jnp.float32)

    def fold(qi, kj, held):
        kb = key_bias[kj]
        top = col_top[kj]
        high = top
        tops = []
        for g in range(8):
            rows = pl.ds(g * 16, 16)
            t = held[rows, :] * scale + kb
            qb = query_bias[qi, rows, :]
            parts = [t[:, i * 128 : (i + 1) * 128] + qb for i in range(4)]
            tops.append(
                jnp.maximum(jnp.maximum(parts[0], parts[1]), jnp.maximum(parts[2], parts[3]))
            )
            both = jnp.concatenate(parts, axis=1)
            scores[qi, kj, rows, :] = both
            high = jnp.maximum(high, jnp.maximum(both[:8], both[8:]))
        total = col_sum[kj] * jnp.exp2(top - high)
        for g in range(8):
            rows = pl.ds(g * 16, 16)
            t = scores[qi, kj, rows, :]
            before = row_top[qi, rows, :]
            now = jnp.maximum(before, tops[g])
            acc = row_sum[qi, rows, :] * jnp.exp2(before - now)
            for i in range(4):
                acc += jnp.exp2(t[:, i * 128 : (i + 1) * 128] - now)
            row_sum[qi, rows, :] = acc
            row_top[qi, rows, :] = now
            total += jnp.exp2(t[:8] - high) + jnp.exp2(t[8:] - high)
        col_sum[kj] = total
        col_top[kj] = high

    def fold_tiles(at, begin, end, last):
        def ahead(n):
            return product(*at(jnp.minimum(n, last - 1)))

        def body(i, carry):
            now, then = ahead(2 * i + 2), ahead(2 * i + 3)
            fold(*at(2 * i), held_even)
            fold(*at(2 * i + 1), held_odd)
            held_even[...] = now
            held_odd[...] = then
            return carry

        if begin == 0:
            held_even[...] = ahead(0)
            held_odd[...] = ahead(1)
        lax.fori_loop(begin // 2, end // 2, body, 0)
        if end % 2:
            fold(*at(end - 1), held_even)

    def wait_chunk(r):
        for s in range(SOURCES):
            landed(queries.at[r, s], qs.at[r, 0], qr.at[r, s])
        landed(keys.at[r, parity * 2 + 1 - c], fs.at[1, r], fr.at[1, r])
        landed(keys.at[r, (1 - parity) * 2 + 1 - c], fs.at[2, r], fr.at[2, r])
        turned[r] = jnp.transpose(keys[r].reshape(512, 256))

    def first_pass(r, begin, count):
        if begin == 0:
            wait_chunk(r)

        def at(n):
            return jnp.minimum(n, r), jnp.where(n <= r, r, n - r - 1)

        fold_tiles(at, begin, begin + count, 2 * r + 1)

    def work_out_routes():
        for side in range(2):
            for pair in range(8):
                every_pair[x, side, pair] = pairs[side, pair]
        for e in range(1, GROUPS):
            other = lax.rem(x + e, GROUPS)
            landed(every_pair.at[other], ps.at[e], pr.at[e])
        before, after, across = (lax.rem(x + k, GROUPS) for k in (3, 1, 2))
        images, routed, bad = route(every_pair, x)
        codes = []
        for s, (d, image, right_place, left_place, _, _) in enumerate(routed):
            far = jnp.where(
                right_place >= 0, within(right_place, ENTER), ENTER + within(left_place, ENTER)
            )
            code = jnp.where(d == 0, image, IMAGES + far)
            for earlier, same in zip(images, codes):
                code = jnp.where(images[s] == earlier, same, code)
            codes.append(code)
            slot_code[s] = code
        _, routed, now = route(every_pair, before)
        bad += now
        entries = [
            (p, jnp.where(d == 1, i, IMAGES + within(m, RELAY))) for d, i, p, _, m, _ in routed
        ]
        for k in range(ENTER):
            enter_code[k] = at_place(entries, k)
        _, routed, now = route(every_pair, after)
        bad += now
        entries = [
            (p, jnp.where(d == 3, i, IMAGES + RELAY + within(m, RELAY)))
            for d, i, _, p, _, m in routed
        ]
        for k in range(ENTER):
            enter_code[ENTER + k] = at_place(entries, k)
        _, routed, now = route(every_pair, across)
        bad += now
        for k in range(RELAY):
            relay_code[k] = at_place([(m, i) for _, i, _, _, m, _ in routed], k)
            relay_code[RELAY + k] = at_place([(m, i) for _, i, _, _, _, m in routed], k)
        misfit[...] = jnp.full(misfit.shape, bad, jnp.int32)

    if narrow:
        for e, device in ((3, right), (1, left), (2, opposite)):
            go(remote(pairs, every_pair.at[x], ps.at[e], pr.at[e], device))
    for r in range(WIDE):
        x_first(r)
    if narrow:
        work_out_routes()
    taken = [0] * CHUNKS
    for step, r, *count in ORDER:
        if step == "first":
            x_first(r)
        elif step == "second":
            x_second(r)
        elif step == "spread":
            select(r)
            spread(r)
        elif step == "keys":
            pass_keys(r)
        elif step == "again":
            pass_again(r)
        elif narrow:
            first_pass(r, taken[r], count[0])
            taken[r] += count[0]
    if not narrow:
        for r in range(CHUNKS):
            wait_chunk(r)
        fold_tiles(lambda n: (n // CHUNKS, n % CHUNKS), 0, CHUNKS**2, CHUNKS**2)

    for kj in range(CHUNKS):
        top = jnp.max(col_top[kj], axis=0, keepdims=True)
        total = jnp.sum(col_sum[kj] * jnp.exp2(col_top[kj] - top), axis=0, keepdims=True)
        log = top + jnp.log2(total)
        for m in range(MEMBERS):
            col_log[member, m, pl.ds(kj, 1), :] = log[:, m * 128 : (m + 1) * 128]
    team = [(1, sibling), (2, beside), (3, diagonal)]

    def mate(e):
        dh, dc = e // 2, e % 2
        return (1 - parity if dh else parity) * 2 + (1 - c if dc else c)

    for e, device in team:
        go(remote(col_log.at[member], col_log.at[member], cs.at[e], cr.at[e], device))

    lane = lax.broadcasted_iota(jnp.int32, (128, 128), 1)
    row_cols = jnp.zeros((128, 128), jnp.float32)
    for qi in range(CHUNKS):
        top = jnp.max(row_top[qi], axis=1, keepdims=True)
        total = jnp.sum(row_sum[qi] * jnp.exp2(row_top[qi] - top), axis=1, keepdims=True)
        row_cols = jnp.where(lane == qi, top + jnp.log2(total), row_cols)
    row_log = jnp.transpose(row_cols)[:8]

    for e, _ in team:
        landed(col_log.at[mate(e)], cs.at[e], cr.at[e])
    own_col = None
    for m in range(MEMBERS):
        logs = [col_log[k, m] for k in range(MEMBERS)]
        top = jnp.maximum(jnp.maximum(logs[0], logs[1]), jnp.maximum(logs[2], logs[3]))
        full = top + jnp.log2(sum(jnp.exp2(v - top) for v in logs))
        col_half[m] = full * 0.5
        own_col = full if m == 0 else jnp.where(member == m, full, own_col)

    def second(qi, carry):
        best = [None] * 8
        for kj in range(CHUNKS):
            halves = [col_half[m, pl.ds(kj, 1), :] for m in range(MEMBERS)]
            for g in range(8):
                t = scores[qi, kj, pl.ds(g * 16, 16), :]
                parts = [t[:, m * 128 : (m + 1) * 128] - halves[m] for m in range(MEMBERS)]
                part = jnp.maximum(
                    jnp.maximum(parts[0], parts[1]), jnp.maximum(parts[2], parts[3])
                )
                best[g] = part if kj == 0 else jnp.maximum(best[g], part)
        for g in range(8):
            rows = pl.ds(g * 16, 16)
            most = jnp.max(best[g], axis=1, keepdims=True)
            best_cols[rows, :] = jnp.where(lane[:16] == qi, most, best_cols[rows, :])
        return carry

    best_cols[...] = jnp.zeros((128, 128), jnp.float32)
    lax.fori_loop(0, CHUNKS, second, 0)
    best = 2.0 * jnp.transpose(best_cols[...])[:8] - row_log

    chunk = lax.broadcasted_iota(jnp.int32, (8, 128), 0)
    lane8 = lax.broadcasted_iota(jnp.int32, (8, 128), 1)
    index = slot_index(z, c, chunk, lane8)
    query_valid = index < query_count
    results = (
        jnp.where(query_valid, row_log * LN2, 0.0),
        jnp.where(index < key_count, own_col * LN2, 0.0),
        jnp.where(query_valid, best * LN2, 0.0),
    )
    for j, value in enumerate(results):
        value = block_transpose(value)
        for s in range(SOURCES):
            sent[s, pl.ds(j, 1), :] = value[s : s + 1]
    for dy in range(4):
        for dk in range(2):
            e = dy * 2 + dk
            to = peer_place(dy, dk)
            if e == 0:
                pltpu.make_async_copy(sent.at[to], got.at[place], or_.at[place]).start()
            else:
                go(remote(sent.at[to], got.at[place], os_.at[e], or_.at[place], peer(dy, dk)))
    for s in range(SOURCES):
        landed(got.at[s], os_.at[0], or_.at[s])
    for s in range(SOURCES):
        for j in range(3):
            out[j, pl.ds(s, 1), :] = got[s, pl.ds(j, 1), :]
    for copy in started:
        copy.wait_send()


def local(descriptors, pairs, counts):
    scale = 2.0 / math.sqrt(descriptors.shape[2]) * LOG2E
    width = descriptors.shape[2]
    bf16, f32 = jnp.bfloat16, jnp.float32
    dma = pltpu.SemaphoreType.DMA
    scratch = [pltpu.VMEM((GROUPS * IMAGES, ROWS, width), bf16) for _ in range(CHUNKS)]
    scratch += [pltpu.VMEM((8, 2, ROWS, width), bf16) for _ in range(CHUNKS)]
    scratch += [
        pltpu.VMEM((CHUNKS, SOURCES, ROWS, width), bf16),
        pltpu.VMEM((CHUNKS, MEMBERS, SOURCES, ROWS, width), bf16),
        pltpu.VMEM((CHUNKS, CHUNKS, 128, 512), f32),
        pltpu.VMEM((CHUNKS, 128, 128), f32),
        pltpu.VMEM((CHUNKS, 128, 128), f32),
        pltpu.VMEM((CHUNKS, 8, 512), f32),
        pltpu.VMEM((CHUNKS, 8, 512), f32),
        pltpu.VMEM((CHUNKS, 1, 512), f32),
        pltpu.VMEM((CHUNKS, 128, 128), f32),
        pltpu.VMEM((MEMBERS, MEMBERS, CHUNKS, 128), f32),
        pltpu.VMEM((MEMBERS, CHUNKS, 128), f32),
        pltpu.VMEM((128, 128), f32),
        pltpu.VMEM((CHUNKS, width, 512), bf16),
        pltpu.VMEM((128, 512), f32),
        pltpu.VMEM((128, 512), f32),
        pltpu.VMEM((8, 8, 128), f32),
        pltpu.VMEM((8, 8, 128), f32),
        dma((CHUNKS,)),
        dma((4, CHUNKS)), dma((4, CHUNKS)),
        dma((CHUNKS, 8)), dma((CHUNKS, 8)),
        dma((CHUNKS, 8)), dma((CHUNKS, 8)),
        dma((3, CHUNKS)), dma((3, CHUNKS)),
        dma((4,)), dma((4,)),
        dma((8,)), dma((8,)),
        pltpu.SMEM((2, 8), jnp.int32), pltpu.SMEM((64,), jnp.int32), dma((2,)),
    ]
    smem, vmem = pltpu.SMEM, pltpu.VMEM

    def call(narrow):
        rooms = list(scratch)
        if narrow:
            rooms[WIDE:CHUNKS] = [vmem((IMAGES, ROWS, width), bf16)] * (CHUNKS - WIDE)
            rooms += [dma((GROUPS,)), dma((GROUPS,))]
            for room in (RELAY, ENTER, RELAY, ENTER):
                rooms += [vmem((2 * room, ROWS, width), bf16)] * CHUNKS
            rooms += [
                smem((GROUPS, 2, 8), jnp.int32),
                smem((2 * RELAY,), jnp.int32),
                smem((2 * ENTER,), jnp.int32),
                smem((IMAGES,), jnp.int32),
            ]
        shapes = [jax.ShapeDtypeStruct((3, 8, 128), f32), jax.ShapeDtypeStruct((1, 1), jnp.int32)]
        count = 2 if narrow else 1
        return pl.pallas_call(
            functools.partial(kernel, scale, narrow),
            out_shape=shapes[:count],
            in_specs=[
                pl.BlockSpec(memory_space=pl.ANY),
                pl.BlockSpec(memory_space=pl.ANY),
                pl.BlockSpec(memory_space=pl.ANY),
            ],
            out_specs=[pl.BlockSpec(memory_space=vmem)] * count,
            scratch_shapes=rooms,
            name="narrow" if narrow else "full",
            compiler_params=pltpu.CompilerParams(
                collective_id=1 if narrow else 0,
                has_side_effects=True,
                vmem_limit_bytes=63 * 1024 * 1024,
            ),
        )(pairs.T, counts, descriptors)

    def split(out):
        return out[0], out[1], out[2]

    out, misfit = call(True)
    return lax.cond(misfit.reshape(()) > 0, lambda _: split(call(False)[0]), split, out)


def solution(mesh):
    torus = Mesh(
        mesh.devices.reshape(mesh.shape["grp"], 4, 4, 2), ("grp", "tile_0", "tile_1", "tile_2")
    )
    return jax.shard_map(
        local,
        mesh=torus,
        in_specs=(P("grp", TILE, None), P("grp", None), P()),
        out_specs=(P("grp", TILE), P("grp", TILE), P("grp", TILE)),
        check_vma=False,
    )
```

```python
import functools
import math

import jax
import jax.numpy as jnp
from jax import lax
from jax.experimental import pallas as pl
from jax.experimental.pallas import tpu as pltpu
from jax.sharding import Mesh
from jax.sharding import PartitionSpec as P

TILE = ("tile_0", "tile_1", "tile_2")
MESH = pl.DeviceIdType.MESH

NEGATIVE = -1e30
CHUNKS = 8
ROWS = 16
GROUPS = 4
IMAGES = 16
SOURCES = 8
MEMBERS = 4
ENTER = 9
RELAY = 4
WIDE = 2
ORDER = (
    ("second", 0), ("first", 2), ("first", 3), ("second", 1), ("first", 4), ("spread", 0),
    ("second", 2), ("first", 5), ("second", 3), ("first", 6), ("spread", 1), ("second", 4),
    ("first", 7), ("spread", 2), ("second", 5), ("keys", 0), ("spread", 3), ("second", 6),
    ("keys", 1), ("spread", 4), ("second", 7), ("again", 0), ("keys", 2), ("spread", 5),
    ("columns", 0, 1), ("rows", 1, 1), ("spread", 6), ("again", 1), ("keys", 3), ("spread", 7),
    ("columns", 1, 2), ("again", 2), ("keys", 4), ("rows", 2, 2), ("columns", 2, 3), ("keys", 5),
    ("again", 3), ("rows", 3, 3), ("columns", 3, 2), ("again", 4), ("keys", 6), ("columns", 3, 2),
    ("rows", 4, 4), ("columns", 4, 2), ("again", 5), ("keys", 7), ("columns", 4, 3),
    ("rows", 5, 5), ("columns", 5, 2), ("again", 6), ("columns", 5, 4), ("rows", 6, 4),
    ("rows", 6, 2), ("again", 7), ("columns", 6, 7), ("rows", 7, 7), ("columns", 7, 8),
)
LOG2E = math.log2(math.e)
LN2 = math.log(2.0)


def slot_index(z, core, chunk, lane):
    outer = jnp.logical_or(z == 0, z == 3)
    low = jnp.where(outer, 0, 1)
    high = jnp.where(outer, 3, 2)
    source = lane // ROWS
    z_source = jnp.where(source % 2 == 0, low, high)
    tile = (source // 2) * 8 + z_source * 2 + core
    return tile * (CHUNKS * ROWS) + chunk * ROWS + lane % ROWS


def block_transpose(x):
    sub = lax.broadcasted_iota(jnp.int32, (8, 128), 0)
    block = lax.broadcasted_iota(jnp.int32, (8, 128), 1) // ROWS
    out = x
    for d in range(8):
        moved = x if d == 0 else pltpu.roll(pltpu.roll(x, ROWS * d, 1), 8 - d, 0)
        out = jnp.where(block == (sub + d) % 8, moved, out)
    return out


def route(pairs, group):
    slots = []
    images = []
    for pair in range(8):
        for side in range(2):
            image = pairs[group, side, pair]
            away = lax.rem(image // IMAGES - group + GROUPS, GROUPS)
            for earlier in images:
                away = jnp.where(image == earlier, 0, away)
            images.append(image)
            slots.append((away, lax.rem(image, IMAGES)))
    one = [[jnp.where(d == k, 1, 0) for d, _ in slots] for k in range(GROUPS)]
    near, far, behind = (sum(one[k]) for k in (1, 2, 3))
    least = jnp.maximum(jnp.maximum(far - RELAY, behind + far - ENTER), 0)
    most = jnp.minimum(jnp.minimum(far, RELAY), ENTER - near)
    by_right = jnp.minimum(jnp.maximum((behind + far - near + 1) // 2, least), most)
    rank = [0] * GROUPS
    routed = []
    for s, (d, image) in enumerate(slots):
        relay_left = rank[2] - by_right
        by_left = jnp.logical_or(d == 3, jnp.logical_and(d == 2, relay_left >= 0))
        from_right = jnp.logical_or(d == 1, jnp.logical_and(d == 2, relay_left < 0))
        right_place = jnp.where(d == 1, rank[1], near + rank[2])
        left_place = jnp.where(d == 3, rank[3], behind + relay_left)
        routed.append(
            (
                d, image,
                jnp.where(from_right, right_place, -1), jnp.where(by_left, left_place, -1),
                jnp.where(jnp.logical_and(d == 2, relay_left < 0), rank[2], -1),
                jnp.where(jnp.logical_and(d == 2, relay_left >= 0), relay_left, -1),
            )
        )
        for k in range(1, GROUPS):
            rank[k] = rank[k] + one[k][s]
    return images, routed, jnp.where(least > most, 1, 0)


def at_place(entries, k):
    return sum(jnp.where(place == k, value, 0) for place, value in entries)


def within(value, count):
    return jnp.minimum(jnp.maximum(value, 0), count - 1)


def kernel(scale, narrow, pairs_in, counts_in, desc, out, *scratch):
    if narrow:
        misfit, scratch = scratch[0], scratch[1:]
        every_pair, relay_code, enter_code, slot_code = scratch[-4:]
        middle, arrived, packed_middle, packed_arrived = (
            scratch[-4 - (4 - k) * CHUNKS : -4 - (3 - k) * CHUNKS] for k in range(4)
        )
        ps, pr = scratch[-4 - 4 * CHUNKS - 2 : -4 - 4 * CHUNKS]
        scratch = scratch[: -4 - 4 * CHUNKS - 2]

    def wide(r):
        return not narrow or r < WIDE

    gathered = scratch[:CHUNKS]
    staged = scratch[CHUNKS : 2 * CHUNKS]
    (
        queries, keys, scores, row_top, row_sum, col_top, col_sum, key_bias, query_bias,
        col_log, col_half, best_lanes, turned, held_even, held_odd, sent, got,
        load_sem, xs, xr, qs, qr, ks, kr, fs, fr, cs, cr, os_, or_,
        pairs, counts, small_sem,
    ) = scratch[2 * CHUNKS :]
    x, y, z, c = (lax.axis_index(a) for a in ("grp",) + TILE)
    right = (lax.rem(x + 1, 4), y, z, c)
    left = (lax.rem(x + 3, 4), y, z, c)
    half = z // 2
    parity = z % 2
    place = y * 2 + half
    member = parity * 2 + c
    z_beside = half * 2 + (1 - parity)
    beside = (x, y, z_beside, c)
    sibling = (x, y, z, 1 - c)
    opposite = (lax.rem(x + 2, 4), y, z, c)
    diagonal = (x, y, z_beside, 1 - c)
    member_beside = (1 - parity) * 2 + c

    def peer(dy, dk):
        return (x, lax.rem(y + dy, 4), z if dk == 0 else 3 - z, c)

    def peer_place(dy, dk):
        return lax.rem(y + dy, 4) * 2 + (half if dk == 0 else 1 - half)

    others = [(dy, dk) for dy in range(4) for dk in range(2) if (dy, dk) != (0, 0)]
    barrier = pltpu.get_barrier_semaphore()
    greeted = [right, left, beside, sibling, diagonal] + [peer(dy, dk) for dy, dk in others]
    if narrow:
        greeted.append(opposite)
    for device in greeted:
        pl.semaphore_signal(barrier, inc=1, device_id=device, device_id_type=MESH)

    small = [
        pltpu.make_async_copy(pairs_in, pairs, small_sem.at[0]),
        pltpu.make_async_copy(counts_in, counts, small_sem.at[1]),
    ]
    for copy in small:
        copy.start()
    loads = [
        pltpu.make_async_copy(
            desc.at[:, pl.ds(r * ROWS, ROWS), :], gathered[r].at[pl.ds(0, IMAGES)], load_sem.at[r]
        )
        for r in range(CHUNKS)
    ]
    for load in loads:
        load.start()

    for copy in small:
        copy.wait()
    p = place
    query_count = counts[pairs[0, p]]
    key_count = counts[pairs[1, p]]
    row_top[...] = jnp.full(row_top.shape, NEGATIVE, jnp.float32)
    row_sum[...] = jnp.zeros(row_sum.shape, jnp.float32)
    col_top[...] = jnp.full(col_top.shape, NEGATIVE, jnp.float32)
    col_sum[...] = jnp.zeros(col_sum.shape, jnp.float32)
    for r in range(CHUNKS):
        lane = lax.broadcasted_iota(jnp.int32, (1, 128), 1)
        for m in range(MEMBERS):
            index = slot_index(half * 2 + m // 2, m % 2, r, lane)
            key_bias[r, :, pl.ds(m * 128, 128)] = jnp.where(index < key_count, 0.0, NEGATIVE)
        sub = lax.broadcasted_iota(jnp.int32, (128, 128), 0)
        query_bias[r] = jnp.where(slot_index(z, c, r, sub) < query_count, 0.0, NEGATIVE)

    pl.semaphore_wait(barrier, len(greeted))

    def remote(src, dst, send, recv, device):
        return pltpu.make_async_remote_copy(
            src_ref=src, dst_ref=dst, send_sem=send, recv_sem=recv,
            device_id=device, device_id_type=MESH,
        )

    started = []

    def go(copy):
        copy.start()
        started.append(copy)

    def own(r):
        return gathered[r].at[pl.ds(0, IMAGES)]

    from_left = lambda r: gathered[r].at[pl.ds(16, 16)]
    from_right = lambda r: gathered[r].at[pl.ds(48, 16)]
    far_low = lambda r: gathered[r].at[pl.ds(32, 8)]
    far_high = lambda r: gathered[r].at[pl.ds(40, 8)]

    def x_first(r):
        loads[r].wait()
        if not wide(r):
            for k in range(2 * RELAY):
                packed_middle[r][k] = gathered[r][relay_code[k]]
            for k, device in ((0, left), (1, right)):
                part = pl.ds(k * RELAY, RELAY)
                go(remote(
                    packed_middle[r].at[part], middle[r].at[part], xs.at[k, r], xr.at[k, r], device
                ))
            return
        go(remote(own(r), from_left(r), xs.at[0, r], xr.at[0, r], right))
        go(remote(own(r), from_right(r), xs.at[1, r], xr.at[1, r], left))

    def landed(ref, send, recv):
        remote(ref, ref, send, recv, right).wait_recv()

    def choose(code, first, other):
        a = first[jnp.minimum(code, IMAGES - 1)]
        b = other[jnp.maximum(code - IMAGES, 0)]
        return lax.select(code < IMAGES, a, b)

    def x_second(r):
        if not wide(r):
            for k in range(2):
                landed(middle[r].at[pl.ds(k * RELAY, RELAY)], xs.at[k, r], xr.at[k, r])
            for k, device in ((0, left), (1, right)):
                for n in range(k * ENTER, (k + 1) * ENTER):
                    packed_arrived[r][n] = choose(enter_code[n], gathered[r], middle[r])
                part = pl.ds(k * ENTER, ENTER)
                go(remote(
                    packed_arrived[r].at[part], arrived[r].at[part],
                    xs.at[2 + k, r], xr.at[2 + k, r], device,
                ))
            return
        landed(from_left(r), xs.at[0, r], xr.at[0, r])
        go(remote(gathered[r].at[pl.ds(16, 8)], far_low(r), xs.at[2, r], xr.at[2, r], right))
        landed(from_right(r), xs.at[1, r], xr.at[1, r])
        go(remote(gathered[r].at[pl.ds(56, 8)], far_high(r), xs.at[3, r], xr.at[3, r], left))

    def select(r):
        if not wide(r):
            for k in range(2):
                landed(arrived[r].at[pl.ds(k * ENTER, ENTER)], xs.at[2 + k, r], xr.at[2 + k, r])
            for pair in range(8):
                for side in range(2):
                    code = slot_code[pair * 2 + side]
                    staged[r][pair, side] = choose(code, gathered[r], arrived[r])
            return
        landed(far_low(r), xs.at[2, r], xr.at[2, r])
        landed(far_high(r), xs.at[3, r], xr.at[3, r])
        for pair in range(8):
            for side in range(2):
                image = pairs[side, pair]
                turn = lax.rem(x + 4 - image // IMAGES, 4)
                staged[r][pair, side] = gathered[r][turn * IMAGES + image % IMAGES]

    def spread(r):
        for dy in range(4):
            for dk in range(2):
                to = peer_place(dy, dk)
                e = dy * 2 + dk
                z_to = z if dk == 0 else 3 - z
                m_to = (z_to % 2) * 2 + c
                q_src, k_src = staged[r].at[to, 0], staged[r].at[to, 1]
                q_dst, k_dst = queries.at[r, place], keys.at[r, m_to, place]
                if e == 0:
                    for copy in (
                        pltpu.make_async_copy(q_src, q_dst, qr.at[r, place]),
                        pltpu.make_async_copy(k_src, k_dst, kr.at[r, place]),
                    ):
                        copy.start()
                else:
                    go(remote(k_src, k_dst, ks.at[r, e], kr.at[r, place], peer(dy, dk)))
                    go(remote(q_src, q_dst, qs.at[r, e], qr.at[r, place], peer(dy, dk)))

    def pass_keys(r):
        for s in range(SOURCES):
            landed(keys.at[r, member, s], ks.at[r, 0], kr.at[r, s])
        block = keys.at[r, member]
        go(remote(block, block, fs.at[0, r], fr.at[0, r], beside))
        go(remote(block, block, fs.at[1, r], fr.at[1, r], sibling))

    def pass_again(r):
        block = keys.at[r, member_beside]
        landed(block, fs.at[0, r], fr.at[0, r])
        go(remote(block, block, fs.at[2, r], fr.at[2, r], sibling))

    def product(qi, kj):
        q = queries[qi].reshape(128, 256)
        return jnp.dot(q, turned[kj], preferred_element_type=jnp.float32)

    def fold(qi, kj, held):
        kb = key_bias[kj]
        top = col_top[kj]
        high = top
        tops = []
        for g in range(8):
            rows = pl.ds(g * 16, 16)
            t = held[rows, :] * scale + kb
            qb = query_bias[qi, rows, :]
            parts = [t[:, i * 128 : (i + 1) * 128] + qb for i in range(4)]
            tops.append(
                jnp.maximum(jnp.maximum(parts[0], parts[1]), jnp.maximum(parts[2], parts[3]))
            )
            both = jnp.concatenate(parts, axis=1)
            scores[qi, kj, rows, :] = both
            high = jnp.maximum(high, jnp.maximum(both[:8], both[8:]))
        total = col_sum[kj] * jnp.exp2(top - high)
        for g in range(8):
            rows = pl.ds(g * 16, 16)
            t = scores[qi, kj, rows, :]
            before = row_top[qi, rows, :]
            now = jnp.maximum(before, tops[g])
            acc = row_sum[qi, rows, :] * jnp.exp2(before - now)
            for i in range(4):
                acc += jnp.exp2(t[:, i * 128 : (i + 1) * 128] - now)
            row_sum[qi, rows, :] = acc
            row_top[qi, rows, :] = now
            total += jnp.exp2(t[:8] - high) + jnp.exp2(t[8:] - high)
        col_sum[kj] = total
        col_top[kj] = high

    def fold_tiles(at, begin, end, last):
        def ahead(n):
            return product(*at(jnp.minimum(n, last - 1)))

        def body(i, carry):
            now, then = ahead(2 * i + 2), ahead(2 * i + 3)
            fold(*at(2 * i), held_even)
            fold(*at(2 * i + 1), held_odd)
            held_even[...] = now
            held_odd[...] = then
            return carry

        if begin == 0:
            held_even[...] = ahead(0)
            held_odd[...] = ahead(1)
        lax.fori_loop(begin // 2, end // 2, body, 0)
        if end % 2:
            fold(*at(end - 1), held_even)

    def wait_rows(r):
        for s in range(SOURCES):
            landed(queries.at[r, s], qs.at[r, 0], qr.at[r, s])

    def wait_columns(r):
        landed(keys.at[r, parity * 2 + 1 - c], fs.at[1, r], fr.at[1, r])
        landed(keys.at[r, (1 - parity) * 2 + 1 - c], fs.at[2, r], fr.at[2, r])
        turned[r] = jnp.transpose(keys[r].reshape(512, 256))

    def fold_rows(r, begin, count):
        if begin == 0:
            wait_rows(r)
        fold_tiles(lambda n: (r, n), begin, begin + count, r)

    def fold_columns(r, begin, count):
        if begin == 0:
            if r == 0:
                wait_rows(r)
            wait_columns(r)
        fold_tiles(lambda n: (n, r), begin, begin + count, r + 1)

    def work_out_routes():
        for side in range(2):
            for pair in range(8):
                every_pair[x, side, pair] = pairs[side, pair]
        for e in range(1, GROUPS):
            other = lax.rem(x + e, GROUPS)
            landed(every_pair.at[other], ps.at[e], pr.at[e])
        before, after, across = (lax.rem(x + k, GROUPS) for k in (3, 1, 2))
        images, routed, bad = route(every_pair, x)
        codes = []
        for s, (d, image, right_place, left_place, _, _) in enumerate(routed):
            far = jnp.where(
                right_place >= 0, within(right_place, ENTER), ENTER + within(left_place, ENTER)
            )
            code = jnp.where(d == 0, image, IMAGES + far)
            for earlier, same in zip(images, codes):
                code = jnp.where(images[s] == earlier, same, code)
            codes.append(code)
            slot_code[s] = code
        _, routed, now = route(every_pair, before)
        bad += now
        entries = [
            (p, jnp.where(d == 1, i, IMAGES + within(m, RELAY))) for d, i, p, _, m, _ in routed
        ]
        for k in range(ENTER):
            enter_code[k] = at_place(entries, k)
        _, routed, now = route(every_pair, after)
        bad += now
        entries = [
            (p, jnp.where(d == 3, i, IMAGES + RELAY + within(m, RELAY)))
            for d, i, _, p, _, m in routed
        ]
        for k in range(ENTER):
            enter_code[ENTER + k] = at_place(entries, k)
        _, routed, now = route(every_pair, across)
        bad += now
        for k in range(RELAY):
            relay_code[k] = at_place([(m, i) for _, i, _, _, m, _ in routed], k)
            relay_code[RELAY + k] = at_place([(m, i) for _, i, _, _, _, m in routed], k)
        misfit[...] = jnp.full(misfit.shape, bad, jnp.int32)

    if narrow:
        for e, device in ((3, right), (1, left), (2, opposite)):
            go(remote(pairs, every_pair.at[x], ps.at[e], pr.at[e], device))
    for r in range(WIDE):
        x_first(r)
    if narrow:
        work_out_routes()
    taken = {"rows": [0] * CHUNKS, "columns": [0] * CHUNKS}
    for step, r, *count in ORDER:
        if step == "first":
            x_first(r)
        elif step == "second":
            x_second(r)
        elif step == "spread":
            select(r)
            spread(r)
        elif step == "keys":
            pass_keys(r)
        elif step == "again":
            pass_again(r)
        elif narrow:
            (fold_rows if step == "rows" else fold_columns)(r, taken[step][r], count[0])
            taken[step][r] += count[0]
    if not narrow:
        for r in range(CHUNKS):
            wait_rows(r)
            wait_columns(r)
        fold_tiles(lambda n: (n // CHUNKS, n % CHUNKS), 0, CHUNKS**2, CHUNKS**2)

    for kj in range(CHUNKS):
        top = jnp.max(col_top[kj], axis=0, keepdims=True)
        total = jnp.sum(col_sum[kj] * jnp.exp2(col_top[kj] - top), axis=0, keepdims=True)
        log = top + jnp.log2(total)
        for m in range(MEMBERS):
            col_log[member, m, pl.ds(kj, 1), :] = log[:, m * 128 : (m + 1) * 128]
    team = [(1, sibling), (2, beside), (3, diagonal)]

    def mate(e):
        dh, dc = e // 2, e % 2
        return (1 - parity if dh else parity) * 2 + (1 - c if dc else c)

    for e, device in team:
        go(remote(col_log.at[member], col_log.at[member], cs.at[e], cr.at[e], device))

    lane = lax.broadcasted_iota(jnp.int32, (128, 128), 1)
    row_cols = jnp.zeros((128, 128), jnp.float32)
    for qi in range(CHUNKS):
        top = jnp.max(row_top[qi], axis=1, keepdims=True)
        total = jnp.sum(row_sum[qi] * jnp.exp2(row_top[qi] - top), axis=1, keepdims=True)
        row_cols = jnp.where(lane == qi, top + jnp.log2(total), row_cols)
    row_log = jnp.transpose(row_cols)[:8]

    for e, _ in team:
        landed(col_log.at[mate(e)], cs.at[e], cr.at[e])
    own_col = None
    for m in range(MEMBERS):
        logs = [col_log[k, m] for k in range(MEMBERS)]
        top = jnp.maximum(jnp.maximum(logs[0], logs[1]), jnp.maximum(logs[2], logs[3]))
        full = top + jnp.log2(sum(jnp.exp2(v - top) for v in logs))
        col_half[m] = full * 0.5
        own_col = full if m == 0 else jnp.where(member == m, full, own_col)

    def second(qi, carry):
        best = [None] * 8
        for kj in range(CHUNKS):
            halves = [col_half[m, pl.ds(kj, 1), :] for m in range(MEMBERS)]
            for g in range(8):
                t = scores[qi, kj, pl.ds(g * 16, 16), :]
                parts = [t[:, m * 128 : (m + 1) * 128] - halves[m] for m in range(MEMBERS)]
                part = jnp.maximum(
                    jnp.maximum(parts[0], parts[1]), jnp.maximum(parts[2], parts[3])
                )
                best[g] = part if kj == 0 else jnp.maximum(best[g], part)
        for g in range(8):
            best_lanes[qi, pl.ds(g * 16, 16), :] = best[g]
        return carry

    lax.fori_loop(0, CHUNKS, second, 0)
    best_cols = jnp.zeros((128, 128), jnp.float32)
    for qi in range(CHUNKS):
        most = jnp.max(best_lanes[qi], axis=1, keepdims=True)
        best_cols = jnp.where(lane == qi, most, best_cols)
    best = 2.0 * jnp.transpose(best_cols)[:8] - row_log

    chunk = lax.broadcasted_iota(jnp.int32, (8, 128), 0)
    lane8 = lax.broadcasted_iota(jnp.int32, (8, 128), 1)
    index = slot_index(z, c, chunk, lane8)
    query_valid = index < query_count
    results = (
        jnp.where(query_valid, row_log * LN2, 0.0),
        jnp.where(index < key_count, own_col * LN2, 0.0),
        jnp.where(query_valid, best * LN2, 0.0),
    )
    for j, value in enumerate(results):
        value = block_transpose(value)
        for s in range(SOURCES):
            sent[s, pl.ds(j, 1), :] = value[s : s + 1]
    before = len(started)
    for dy in range(4):
        for dk in range(2):
            e = dy * 2 + dk
            to = peer_place(dy, dk)
            if e == 0:
                pltpu.make_async_copy(sent.at[to], got.at[place], or_.at[place]).start()
            else:
                go(remote(sent.at[to], got.at[place], os_.at[e], or_.at[place], peer(dy, dk)))
    for copy in started[:before]:
        copy.wait_send()
    for s in range(SOURCES):
        landed(got.at[s], os_.at[0], or_.at[s])
    for s in range(SOURCES):
        for j in range(3):
            out[j, pl.ds(s, 1), :] = got[s, pl.ds(j, 1), :]
    for copy in started[before:]:
        copy.wait_send()


def local(descriptors, pairs, counts):
    scale = 2.0 / math.sqrt(descriptors.shape[2]) * LOG2E
    width = descriptors.shape[2]
    bf16, f32 = jnp.bfloat16, jnp.float32
    dma = pltpu.SemaphoreType.DMA
    scratch = [pltpu.VMEM((GROUPS * IMAGES, ROWS, width), bf16) for _ in range(CHUNKS)]
    scratch += [pltpu.VMEM((8, 2, ROWS, width), bf16) for _ in range(CHUNKS)]
    scratch += [
        pltpu.VMEM((CHUNKS, SOURCES, ROWS, width), bf16),
        pltpu.VMEM((CHUNKS, MEMBERS, SOURCES, ROWS, width), bf16),
        pltpu.VMEM((CHUNKS, CHUNKS, 128, 512), f32),
        pltpu.VMEM((CHUNKS, 128, 128), f32),
        pltpu.VMEM((CHUNKS, 128, 128), f32),
        pltpu.VMEM((CHUNKS, 8, 512), f32),
        pltpu.VMEM((CHUNKS, 8, 512), f32),
        pltpu.VMEM((CHUNKS, 1, 512), f32),
        pltpu.VMEM((CHUNKS, 128, 128), f32),
        pltpu.VMEM((MEMBERS, MEMBERS, CHUNKS, 128), f32),
        pltpu.VMEM((MEMBERS, CHUNKS, 128), f32),
        pltpu.VMEM((CHUNKS, 128, 128), f32),
        pltpu.VMEM((CHUNKS, width, 512), bf16),
        pltpu.VMEM((128, 512), f32),
        pltpu.VMEM((128, 512), f32),
        pltpu.VMEM((8, 8, 128), f32),
        pltpu.VMEM((8, 8, 128), f32),
        dma((CHUNKS,)),
        dma((4, CHUNKS)), dma((4, CHUNKS)),
        dma((CHUNKS, 8)), dma((CHUNKS, 8)),
        dma((CHUNKS, 8)), dma((CHUNKS, 8)),
        dma((3, CHUNKS)), dma((3, CHUNKS)),
        dma((4,)), dma((4,)),
        dma((8,)), dma((8,)),
        pltpu.SMEM((2, 8), jnp.int32), pltpu.SMEM((64,), jnp.int32), dma((2,)),
    ]
    smem, vmem = pltpu.SMEM, pltpu.VMEM

    def call(narrow):
        rooms = list(scratch)
        if narrow:
            rooms[WIDE:CHUNKS] = [vmem((IMAGES, ROWS, width), bf16)] * (CHUNKS - WIDE)
            rooms += [dma((GROUPS,)), dma((GROUPS,))]
            for room in (RELAY, ENTER, RELAY, ENTER):
                rooms += [vmem((2 * room, ROWS, width), bf16)] * CHUNKS
            rooms += [
                smem((GROUPS, 2, 8), jnp.int32),
                smem((2 * RELAY,), jnp.int32),
                smem((2 * ENTER,), jnp.int32),
                smem((IMAGES,), jnp.int32),
            ]
        shapes = [jax.ShapeDtypeStruct((3, 8, 128), f32), jax.ShapeDtypeStruct((1, 1), jnp.int32)]
        count = 2 if narrow else 1
        return pl.pallas_call(
            functools.partial(kernel, scale, narrow),
            out_shape=shapes[:count],
            in_specs=[
                pl.BlockSpec(memory_space=pl.ANY),
                pl.BlockSpec(memory_space=pl.ANY),
                pl.BlockSpec(memory_space=pl.ANY),
            ],
            out_specs=[pl.BlockSpec(memory_space=vmem)] * count,
            scratch_shapes=rooms,
            name="narrow" if narrow else "full",
            compiler_params=pltpu.CompilerParams(
                collective_id=1 if narrow else 0,
                has_side_effects=True,
                vmem_limit_bytes=63 * 1024 * 1024,
            ),
        )(pairs.T, counts, descriptors)

    def split(out):
        return out[0], out[1], out[2]

    out, misfit = call(True)
    return lax.cond(misfit.reshape(()) > 0, lambda _: split(call(False)[0]), split, out)


def solution(mesh):
    torus = Mesh(
        mesh.devices.reshape(mesh.shape["grp"], 4, 4, 2), ("grp", "tile_0", "tile_1", "tile_2")
    )
    return jax.shard_map(
        local,
        mesh=torus,
        in_specs=(P("grp", TILE, None), P("grp", None), P()),
        out_specs=(P("grp", TILE), P("grp", TILE), P("grp", TILE)),
        check_vma=False,
    )
```

```python
import functools
import math

import jax
import jax.numpy as jnp
from jax import lax
from jax.experimental import pallas as pl
from jax.experimental.pallas import tpu as pltpu
from jax.sharding import Mesh
from jax.sharding import PartitionSpec as P

TILE = ("tile_0", "tile_1", "tile_2")
MESH = pl.DeviceIdType.MESH

NEGATIVE = -1e30
CHUNKS = 8
ROWS = 16
GROUPS = 4
IMAGES = 16
SOURCES = 8
MEMBERS = 4
ENTER = 9
RELAY = 4
WIDE = 2
ORDER = (
    ("second", 0), ("first", 2), ("first", 3), ("second", 1), ("first", 4), ("spread", 0),
    ("second", 2), ("first", 5), ("second", 3), ("first", 6), ("spread", 1), ("second", 4),
    ("first", 7), ("spread", 2), ("second", 5), ("keys", 0), ("spread", 3), ("second", 6),
    ("keys", 1), ("spread", 4), ("second", 7), ("again", 0), ("keys", 2), ("spread", 5),
    ("fold", 0, 2), ("spread", 6), ("keys", 3), ("again", 1), ("spread", 7), ("fold", 1, 2),
    ("keys", 4), ("again", 2), ("fold", 1, 2), ("fold", 2, 2), ("keys", 5), ("again", 3),
    ("fold", 2, 4), ("fold", 3, 2), ("keys", 6), ("again", 4), ("fold", 3, 6), ("fold", 4, 2),
    ("keys", 7), ("again", 5), ("fold", 4, 8), ("fold", 5, 2), ("again", 6), ("fold", 5, 10),
    ("fold", 6, 2), ("again", 7), ("fold", 6, 12), ("fold", 7, 8),
)
LOG2E = math.log2(math.e)
LN2 = math.log(2.0)


def slot_index(z, core, chunk, lane):
    outer = jnp.logical_or(z == 0, z == 3)
    low = jnp.where(outer, 0, 1)
    high = jnp.where(outer, 3, 2)
    source = lane // ROWS
    z_source = jnp.where(source % 2 == 0, low, high)
    tile = (source // 2) * 8 + z_source * 2 + core
    return tile * (CHUNKS * ROWS) + chunk * ROWS + lane % ROWS


def block_transpose(x):
    sub = lax.broadcasted_iota(jnp.int32, (8, 128), 0)
    block = lax.broadcasted_iota(jnp.int32, (8, 128), 1) // ROWS
    out = x
    for d in range(8):
        moved = x if d == 0 else pltpu.roll(pltpu.roll(x, ROWS * d, 1), 8 - d, 0)
        out = jnp.where(block == (sub + d) % 8, moved, out)
    return out


def route(pairs, group):
    slots = []
    images = []
    for pair in range(8):
        for side in range(2):
            image = pairs[group, side, pair]
            away = lax.rem(image // IMAGES - group + GROUPS, GROUPS)
            for earlier in images:
                away = jnp.where(image == earlier, 0, away)
            images.append(image)
            slots.append((away, lax.rem(image, IMAGES)))
    one = [[jnp.where(d == k, 1, 0) for d, _ in slots] for k in range(GROUPS)]
    near, far, behind = (sum(one[k]) for k in (1, 2, 3))
    least = jnp.maximum(jnp.maximum(far - RELAY, behind + far - ENTER), 0)
    most = jnp.minimum(jnp.minimum(far, RELAY), ENTER - near)
    by_right = jnp.minimum(jnp.maximum((behind + far - near + 1) // 2, least), most)
    rank = [0] * GROUPS
    routed = []
    for s, (d, image) in enumerate(slots):
        relay_left = rank[2] - by_right
        by_left = jnp.logical_or(d == 3, jnp.logical_and(d == 2, relay_left >= 0))
        from_right = jnp.logical_or(d == 1, jnp.logical_and(d == 2, relay_left < 0))
        right_place = jnp.where(d == 1, rank[1], near + rank[2])
        left_place = jnp.where(d == 3, rank[3], behind + relay_left)
        routed.append(
            (
                d, image,
                jnp.where(from_right, right_place, -1), jnp.where(by_left, left_place, -1),
                jnp.where(jnp.logical_and(d == 2, relay_left < 0), rank[2], -1),
                jnp.where(jnp.logical_and(d == 2, relay_left >= 0), relay_left, -1),
            )
        )
        for k in range(1, GROUPS):
            rank[k] = rank[k] + one[k][s]
    return images, routed, jnp.where(least > most, 1, 0)


def at_place(entries, k):
    return sum(jnp.where(place == k, value, 0) for place, value in entries)


def within(value, count):
    return jnp.minimum(jnp.maximum(value, 0), count - 1)


def kernel(scale, narrow, pairs_in, counts_in, desc, out, *scratch):
    if narrow:
        misfit, scratch = scratch[0], scratch[1:]
        every_pair, relay_code, enter_code, slot_code = scratch[-4:]
        middle, arrived, packed_middle, packed_arrived = (
            scratch[-4 - (4 - k) * CHUNKS : -4 - (3 - k) * CHUNKS] for k in range(4)
        )
        ps, pr = scratch[-4 - 4 * CHUNKS - 2 : -4 - 4 * CHUNKS]
        scratch = scratch[: -4 - 4 * CHUNKS - 2]

    def wide(r):
        return not narrow or r < WIDE

    gathered = scratch[:CHUNKS]
    staged = scratch[CHUNKS : 2 * CHUNKS]
    (
        queries, keys, scores, row_top, row_sum, col_top, col_sum, key_bias, query_bias,
        col_log, col_half, best_lanes, turned, held_even, held_odd, sent, got,
        load_sem, xs, xr, qs, qr, ks, kr, fs, fr, cs, cr, os_, or_,
        pairs, counts, small_sem,
    ) = scratch[2 * CHUNKS :]
    x, y, z, c = (lax.axis_index(a) for a in ("grp",) + TILE)
    right = (lax.rem(x + 1, 4), y, z, c)
    left = (lax.rem(x + 3, 4), y, z, c)
    half = z // 2
    parity = z % 2
    place = y * 2 + half
    member = parity * 2 + c
    z_beside = half * 2 + (1 - parity)
    beside = (x, y, z_beside, c)
    sibling = (x, y, z, 1 - c)
    opposite = (lax.rem(x + 2, 4), y, z, c)
    diagonal = (x, y, z_beside, 1 - c)
    member_beside = (1 - parity) * 2 + c

    def peer(dy, dk):
        return (x, lax.rem(y + dy, 4), z if dk == 0 else 3 - z, c)

    def peer_place(dy, dk):
        return lax.rem(y + dy, 4) * 2 + (half if dk == 0 else 1 - half)

    others = [(dy, dk) for dy in range(4) for dk in range(2) if (dy, dk) != (0, 0)]
    barrier = pltpu.get_barrier_semaphore()
    greeted = [right, left, beside, sibling, diagonal] + [peer(dy, dk) for dy, dk in others]
    if narrow:
        greeted.append(opposite)
    for device in greeted:
        pl.semaphore_signal(barrier, inc=1, device_id=device, device_id_type=MESH)

    small = [
        pltpu.make_async_copy(pairs_in, pairs, small_sem.at[0]),
        pltpu.make_async_copy(counts_in, counts, small_sem.at[1]),
    ]
    for copy in small:
        copy.start()
    loads = [
        pltpu.make_async_copy(
            desc.at[:, pl.ds(r * ROWS, ROWS), :], gathered[r].at[pl.ds(0, IMAGES)], load_sem.at[r]
        )
        for r in range(CHUNKS)
    ]
    for load in loads:
        load.start()

    for copy in small:
        copy.wait()
    p = place
    query_count = counts[pairs[0, p]]
    key_count = counts[pairs[1, p]]
    row_top[...] = jnp.full(row_top.shape, NEGATIVE, jnp.float32)
    row_sum[...] = jnp.zeros(row_sum.shape, jnp.float32)
    col_top[...] = jnp.full(col_top.shape, NEGATIVE, jnp.float32)
    col_sum[...] = jnp.zeros(col_sum.shape, jnp.float32)
    for r in range(CHUNKS):
        lane = lax.broadcasted_iota(jnp.int32, (1, 128), 1)
        for m in range(MEMBERS):
            index = slot_index(half * 2 + m // 2, m % 2, r, lane)
            key_bias[r, :, pl.ds(m * 128, 128)] = jnp.where(index < key_count, 0.0, NEGATIVE)
        sub = lax.broadcasted_iota(jnp.int32, (128, 128), 0)
        query_bias[r] = jnp.where(slot_index(z, c, r, sub) < query_count, 0.0, NEGATIVE)

    pl.semaphore_wait(barrier, len(greeted))

    def remote(src, dst, send, recv, device):
        return pltpu.make_async_remote_copy(
            src_ref=src, dst_ref=dst, send_sem=send, recv_sem=recv,
            device_id=device, device_id_type=MESH,
        )

    started = []

    def go(copy):
        copy.start()
        started.append(copy)

    def own(r):
        return gathered[r].at[pl.ds(0, IMAGES)]

    from_left = lambda r: gathered[r].at[pl.ds(16, 16)]
    from_right = lambda r: gathered[r].at[pl.ds(48, 16)]
    far_low = lambda r: gathered[r].at[pl.ds(32, 8)]
    far_high = lambda r: gathered[r].at[pl.ds(40, 8)]

    def x_first(r):
        loads[r].wait()
        if not wide(r):
            for k in range(2 * RELAY):
                packed_middle[r][k] = gathered[r][relay_code[k]]
            for k, device in ((0, left), (1, right)):
                part = pl.ds(k * RELAY, RELAY)
                go(remote(
                    packed_middle[r].at[part], middle[r].at[part], xs.at[k, r], xr.at[k, r], device
                ))
            return
        go(remote(own(r), from_left(r), xs.at[0, r], xr.at[0, r], right))
        go(remote(own(r), from_right(r), xs.at[1, r], xr.at[1, r], left))

    def landed(ref, send, recv):
        remote(ref, ref, send, recv, right).wait_recv()

    def choose(code, first, other):
        a = first[jnp.minimum(code, IMAGES - 1)]
        b = other[jnp.maximum(code - IMAGES, 0)]
        return lax.select(code < IMAGES, a, b)

    def x_second(r):
        if not wide(r):
            for k in range(2):
                landed(middle[r].at[pl.ds(k * RELAY, RELAY)], xs.at[k, r], xr.at[k, r])
            for k, device in ((0, left), (1, right)):
                for n in range(k * ENTER, (k + 1) * ENTER):
                    packed_arrived[r][n] = choose(enter_code[n], gathered[r], middle[r])
                part = pl.ds(k * ENTER, ENTER)
                go(remote(
                    packed_arrived[r].at[part], arrived[r].at[part],
                    xs.at[2 + k, r], xr.at[2 + k, r], device,
                ))
            return
        landed(from_left(r), xs.at[0, r], xr.at[0, r])
        go(remote(gathered[r].at[pl.ds(16, 8)], far_low(r), xs.at[2, r], xr.at[2, r], right))
        landed(from_right(r), xs.at[1, r], xr.at[1, r])
        go(remote(gathered[r].at[pl.ds(56, 8)], far_high(r), xs.at[3, r], xr.at[3, r], left))

    def select(r):
        if not wide(r):
            for k in range(2):
                landed(arrived[r].at[pl.ds(k * ENTER, ENTER)], xs.at[2 + k, r], xr.at[2 + k, r])
            for pair in range(8):
                for side in range(2):
                    code = slot_code[pair * 2 + side]
                    staged[r][pair, side] = choose(code, gathered[r], arrived[r])
            return
        landed(far_low(r), xs.at[2, r], xr.at[2, r])
        landed(far_high(r), xs.at[3, r], xr.at[3, r])
        for pair in range(8):
            for side in range(2):
                image = pairs[side, pair]
                turn = lax.rem(x + 4 - image // IMAGES, 4)
                staged[r][pair, side] = gathered[r][turn * IMAGES + image % IMAGES]

    def spread(r):
        for dy in range(4):
            for dk in range(2):
                to = peer_place(dy, dk)
                e = dy * 2 + dk
                z_to = z if dk == 0 else 3 - z
                m_to = (z_to % 2) * 2 + c
                q_src, k_src = staged[r].at[to, 0], staged[r].at[to, 1]
                q_dst, k_dst = queries.at[r, place], keys.at[r, m_to, place]
                if e == 0:
                    for copy in (
                        pltpu.make_async_copy(q_src, q_dst, qr.at[r, place]),
                        pltpu.make_async_copy(k_src, k_dst, kr.at[r, place]),
                    ):
                        copy.start()
                else:
                    go(remote(k_src, k_dst, ks.at[r, e], kr.at[r, place], peer(dy, dk)))
                    go(remote(q_src, q_dst, qs.at[r, e], qr.at[r, place], peer(dy, dk)))

    def pass_keys(r):
        for s in range(SOURCES):
            landed(keys.at[r, member, s], ks.at[r, 0], kr.at[r, s])
        block = keys.at[r, member]
        go(remote(block, block, fs.at[0, r], fr.at[0, r], beside))
        go(remote(block, block, fs.at[1, r], fr.at[1, r], sibling))

    def pass_again(r):
        block = keys.at[r, member_beside]
        landed(block, fs.at[0, r], fr.at[0, r])
        go(remote(block, block, fs.at[2, r], fr.at[2, r], sibling))

    def product(qi, kj):
        q = queries[qi].reshape(128, 256)
        return jnp.dot(q, turned[kj], preferred_element_type=jnp.float32)

    def fold(qi, kj, held):
        kb = key_bias[kj]
        top = col_top[kj]
        high = top
        tops = []
        for g in range(8):
            rows = pl.ds(g * 16, 16)
            t = held[rows, :] * scale + kb
            qb = query_bias[qi, rows, :]
            parts = [t[:, i * 128 : (i + 1) * 128] + qb for i in range(4)]
            tops.append(
                jnp.maximum(jnp.maximum(parts[0], parts[1]), jnp.maximum(parts[2], parts[3]))
            )
            both = jnp.concatenate(parts, axis=1)
            scores[qi, kj, rows, :] = both
            high = jnp.maximum(high, jnp.maximum(both[:8], both[8:]))
        total = col_sum[kj] * jnp.exp2(top - high)
        for g in range(8):
            rows = pl.ds(g * 16, 16)
            t = scores[qi, kj, rows, :]
            before = row_top[qi, rows, :]
            now = jnp.maximum(before, tops[g])
            acc = row_sum[qi, rows, :] * jnp.exp2(before - now)
            for i in range(4):
                acc += jnp.exp2(t[:, i * 128 : (i + 1) * 128] - now)
            row_sum[qi, rows, :] = acc
            row_top[qi, rows, :] = now
            total += jnp.exp2(t[:8] - high) + jnp.exp2(t[8:] - high)
        col_sum[kj] = total
        col_top[kj] = high

    def fold_tiles(at, begin, end, last):
        def ahead(n):
            return product(*at(jnp.minimum(n, last - 1)))

        def body(i, carry):
            now, then = ahead(2 * i + 2), ahead(2 * i + 3)
            fold(*at(2 * i), held_even)
            fold(*at(2 * i + 1), held_odd)
            held_even[...] = now
            held_odd[...] = then
            return carry

        if begin == 0:
            held_even[...] = ahead(0)
            held_odd[...] = ahead(1)
        lax.fori_loop(begin // 2, end // 2, body, 0)
        if end % 2:
            fold(*at(end - 1), held_even)

    def wait_rows(r):
        for s in range(SOURCES):
            landed(queries.at[r, s], qs.at[r, 0], qr.at[r, s])

    def wait_columns(r):
        landed(keys.at[r, parity * 2 + 1 - c], fs.at[1, r], fr.at[1, r])
        landed(keys.at[r, (1 - parity) * 2 + 1 - c], fs.at[2, r], fr.at[2, r])
        turned[r] = jnp.transpose(keys[r].reshape(512, 256))

    def fold_chunk(r, begin, count):
        final = r == CHUNKS - 1
        if begin == 0:
            if r == 0:
                wait_rows(r)
            wait_columns(r)
            if not final:
                wait_rows(r + 1)

        def at(n):
            return jnp.where(n <= r, n, r + 1), jnp.where(n <= r, r, n - r - 1)

        fold_tiles(at, begin, begin + count, r + 1 if final else 2 * r + 2)

    def work_out_routes():
        for side in range(2):
            for pair in range(8):
                every_pair[x, side, pair] = pairs[side, pair]
        for e in range(1, GROUPS):
            other = lax.rem(x + e, GROUPS)
            landed(every_pair.at[other], ps.at[e], pr.at[e])
        before, after, across = (lax.rem(x + k, GROUPS) for k in (3, 1, 2))
        images, routed, bad = route(every_pair, x)
        codes = []
        for s, (d, image, right_place, left_place, _, _) in enumerate(routed):
            far = jnp.where(
                right_place >= 0, within(right_place, ENTER), ENTER + within(left_place, ENTER)
            )
            code = jnp.where(d == 0, image, IMAGES + far)
            for earlier, same in zip(images, codes):
                code = jnp.where(images[s] == earlier, same, code)
            codes.append(code)
            slot_code[s] = code
        _, routed, now = route(every_pair, before)
        bad += now
        entries = [
            (p, jnp.where(d == 1, i, IMAGES + within(m, RELAY))) for d, i, p, _, m, _ in routed
        ]
        for k in range(ENTER):
            enter_code[k] = at_place(entries, k)
        _, routed, now = route(every_pair, after)
        bad += now
        entries = [
            (p, jnp.where(d == 3, i, IMAGES + RELAY + within(m, RELAY)))
            for d, i, _, p, _, m in routed
        ]
        for k in range(ENTER):
            enter_code[ENTER + k] = at_place(entries, k)
        _, routed, now = route(every_pair, across)
        bad += now
        for k in range(RELAY):
            relay_code[k] = at_place([(m, i) for _, i, _, _, m, _ in routed], k)
            relay_code[RELAY + k] = at_place([(m, i) for _, i, _, _, _, m in routed], k)
        misfit[...] = jnp.full(misfit.shape, bad, jnp.int32)

    if narrow:
        for e, device in ((3, right), (1, left), (2, opposite)):
            go(remote(pairs, every_pair.at[x], ps.at[e], pr.at[e], device))
    for r in range(WIDE):
        x_first(r)
    if narrow:
        work_out_routes()
    taken = [0] * CHUNKS
    for step, r, *count in ORDER:
        if step == "first":
            x_first(r)
        elif step == "second":
            x_second(r)
        elif step == "spread":
            select(r)
            spread(r)
        elif step == "keys":
            pass_keys(r)
        elif step == "again":
            pass_again(r)
        elif narrow:
            fold_chunk(r, taken[r], count[0])
            taken[r] += count[0]
    if not narrow:
        for r in range(CHUNKS):
            wait_rows(r)
            wait_columns(r)
        fold_tiles(lambda n: (n // CHUNKS, n % CHUNKS), 0, CHUNKS**2, CHUNKS**2)

    for kj in range(CHUNKS):
        top = jnp.max(col_top[kj], axis=0, keepdims=True)
        total = jnp.sum(col_sum[kj] * jnp.exp2(col_top[kj] - top), axis=0, keepdims=True)
        log = top + jnp.log2(total)
        for m in range(MEMBERS):
            col_log[member, m, pl.ds(kj, 1), :] = log[:, m * 128 : (m + 1) * 128]
    team = [(1, sibling), (2, beside), (3, diagonal)]

    def mate(e):
        dh, dc = e // 2, e % 2
        return (1 - parity if dh else parity) * 2 + (1 - c if dc else c)

    for e, device in team:
        go(remote(col_log.at[member], col_log.at[member], cs.at[e], cr.at[e], device))

    lane = lax.broadcasted_iota(jnp.int32, (128, 128), 1)
    row_cols = jnp.zeros((128, 128), jnp.float32)
    for qi in range(CHUNKS):
        top = jnp.max(row_top[qi], axis=1, keepdims=True)
        total = jnp.sum(row_sum[qi] * jnp.exp2(row_top[qi] - top), axis=1, keepdims=True)
        row_cols = jnp.where(lane == qi, top + jnp.log2(total), row_cols)
    row_log = jnp.transpose(row_cols)[:8]

    for e, _ in team:
        landed(col_log.at[mate(e)], cs.at[e], cr.at[e])
    own_col = None
    for m in range(MEMBERS):
        logs = [col_log[k, m] for k in range(MEMBERS)]
        top = jnp.maximum(jnp.maximum(logs[0], logs[1]), jnp.maximum(logs[2], logs[3]))
        full = top + jnp.log2(sum(jnp.exp2(v - top) for v in logs))
        col_half[m] = full * 0.5
        own_col = full if m == 0 else jnp.where(member == m, full, own_col)

    def second(qi, carry):
        best = [None] * 8
        for kj in range(CHUNKS):
            halves = [col_half[m, pl.ds(kj, 1), :] for m in range(MEMBERS)]
            for g in range(8):
                t = scores[qi, kj, pl.ds(g * 16, 16), :]
                parts = [t[:, m * 128 : (m + 1) * 128] - halves[m] for m in range(MEMBERS)]
                part = jnp.maximum(
                    jnp.maximum(parts[0], parts[1]), jnp.maximum(parts[2], parts[3])
                )
                best[g] = part if kj == 0 else jnp.maximum(best[g], part)
        for g in range(8):
            best_lanes[qi, pl.ds(g * 16, 16), :] = best[g]
        return carry

    lax.fori_loop(0, CHUNKS, second, 0)
    best_cols = jnp.zeros((128, 128), jnp.float32)
    for qi in range(CHUNKS):
        most = jnp.max(best_lanes[qi], axis=1, keepdims=True)
        best_cols = jnp.where(lane == qi, most, best_cols)
    best = 2.0 * jnp.transpose(best_cols)[:8] - row_log

    chunk = lax.broadcasted_iota(jnp.int32, (8, 128), 0)
    lane8 = lax.broadcasted_iota(jnp.int32, (8, 128), 1)
    index = slot_index(z, c, chunk, lane8)
    query_valid = index < query_count
    results = (
        jnp.where(query_valid, row_log * LN2, 0.0),
        jnp.where(index < key_count, own_col * LN2, 0.0),
        jnp.where(query_valid, best * LN2, 0.0),
    )
    for j, value in enumerate(results):
        value = block_transpose(value)
        for s in range(SOURCES):
            sent[s, pl.ds(j, 1), :] = value[s : s + 1]
    before = len(started)
    for dy in range(4):
        for dk in range(2):
            e = dy * 2 + dk
            to = peer_place(dy, dk)
            if e == 0:
                pltpu.make_async_copy(sent.at[to], got.at[place], or_.at[place]).start()
            else:
                go(remote(sent.at[to], got.at[place], os_.at[e], or_.at[place], peer(dy, dk)))
    for copy in started[:before]:
        copy.wait_send()
    for s in range(SOURCES):
        landed(got.at[s], os_.at[0], or_.at[s])
    for s in range(SOURCES):
        for j in range(3):
            out[j, pl.ds(s, 1), :] = got[s, pl.ds(j, 1), :]
    for copy in started[before:]:
        copy.wait_send()


def local(descriptors, pairs, counts):
    scale = 2.0 / math.sqrt(descriptors.shape[2]) * LOG2E
    width = descriptors.shape[2]
    bf16, f32 = jnp.bfloat16, jnp.float32
    dma = pltpu.SemaphoreType.DMA
    scratch = [pltpu.VMEM((GROUPS * IMAGES, ROWS, width), bf16) for _ in range(CHUNKS)]
    scratch += [pltpu.VMEM((8, 2, ROWS, width), bf16) for _ in range(CHUNKS)]
    scratch += [
        pltpu.VMEM((CHUNKS, SOURCES, ROWS, width), bf16),
        pltpu.VMEM((CHUNKS, MEMBERS, SOURCES, ROWS, width), bf16),
        pltpu.VMEM((CHUNKS, CHUNKS, 128, 512), f32),
        pltpu.VMEM((CHUNKS, 128, 128), f32),
        pltpu.VMEM((CHUNKS, 128, 128), f32),
        pltpu.VMEM((CHUNKS, 8, 512), f32),
        pltpu.VMEM((CHUNKS, 8, 512), f32),
        pltpu.VMEM((CHUNKS, 1, 512), f32),
        pltpu.VMEM((CHUNKS, 128, 128), f32),
        pltpu.VMEM((MEMBERS, MEMBERS, CHUNKS, 128), f32),
        pltpu.VMEM((MEMBERS, CHUNKS, 128), f32),
        pltpu.VMEM((CHUNKS, 128, 128), f32),
        pltpu.VMEM((CHUNKS, width, 512), bf16),
        pltpu.VMEM((128, 512), f32),
        pltpu.VMEM((128, 512), f32),
        pltpu.VMEM((8, 8, 128), f32),
        pltpu.VMEM((8, 8, 128), f32),
        dma((CHUNKS,)),
        dma((4, CHUNKS)), dma((4, CHUNKS)),
        dma((CHUNKS, 8)), dma((CHUNKS, 8)),
        dma((CHUNKS, 8)), dma((CHUNKS, 8)),
        dma((3, CHUNKS)), dma((3, CHUNKS)),
        dma((4,)), dma((4,)),
        dma((8,)), dma((8,)),
        pltpu.SMEM((2, 8), jnp.int32), pltpu.SMEM((64,), jnp.int32), dma((2,)),
    ]
    smem, vmem = pltpu.SMEM, pltpu.VMEM

    def call(narrow):
        rooms = list(scratch)
        if narrow:
            rooms[WIDE:CHUNKS] = [vmem((IMAGES, ROWS, width), bf16)] * (CHUNKS - WIDE)
            rooms += [dma((GROUPS,)), dma((GROUPS,))]
            for room in (RELAY, ENTER, RELAY, ENTER):
                rooms += [vmem((2 * room, ROWS, width), bf16)] * CHUNKS
            rooms += [
                smem((GROUPS, 2, 8), jnp.int32),
                smem((2 * RELAY,), jnp.int32),
                smem((2 * ENTER,), jnp.int32),
                smem((IMAGES,), jnp.int32),
            ]
        shapes = [jax.ShapeDtypeStruct((3, 8, 128), f32), jax.ShapeDtypeStruct((1, 1), jnp.int32)]
        count = 2 if narrow else 1
        return pl.pallas_call(
            functools.partial(kernel, scale, narrow),
            out_shape=shapes[:count],
            in_specs=[
                pl.BlockSpec(memory_space=pl.ANY),
                pl.BlockSpec(memory_space=pl.ANY),
                pl.BlockSpec(memory_space=pl.ANY),
            ],
            out_specs=[pl.BlockSpec(memory_space=vmem)] * count,
            scratch_shapes=rooms,
            name="narrow" if narrow else "full",
            compiler_params=pltpu.CompilerParams(
                collective_id=1 if narrow else 0,
                has_side_effects=True,
                vmem_limit_bytes=63 * 1024 * 1024,
            ),
        )(pairs.T, counts, descriptors)

    def split(out):
        return out[0], out[1], out[2]

    out, misfit = call(True)
    return lax.cond(misfit.reshape(()) > 0, lambda _: split(call(False)[0]), split, out)


def solution(mesh):
    torus = Mesh(
        mesh.devices.reshape(mesh.shape["grp"], 4, 4, 2), ("grp", "tile_0", "tile_1", "tile_2")
    )
    return jax.shard_map(
        local,
        mesh=torus,
        in_specs=(P("grp", TILE, None), P("grp", None), P()),
        out_specs=(P("grp", TILE), P("grp", TILE), P("grp", TILE)),
        check_vma=False,
    )
```
